512 devices in a mesh: groups: 2 (over y), cells: 128 (over z, x), side: 2 (over core).
Axes of the slice: x: 4, y: 2, z: 32, core: 2. Of those that a mesh axis runs over, the one named last changes fastest.
The devices are a block of a 4x8x32 slice.
Arguments:
- datasets: float32 [2, 2000, 131072], P('side', None, ('groups', 'cells')), parts along dimension 2, may hold values from -6 to 6
- sketch: float32 [64, 131072], P(None, ('groups', 'cells')), parts along dimension 1, may hold values from -6 to 6
Outputs:
- factors: float32 [2, 64, 131072], P('side', None, ('groups', 'cells')), parts along dimension 2
The draws below stay inside these ranges and needn't reach their ends.
There are 2 independent parts, one for each index of `groups`. The reference program is written for one: setup_inputs(seed, part) draws one part's arguments, and reference() takes and returns one part's arrays. A program takes and returns all parts, laid end to end along the dimension named above; each array names one. Nothing has to cross between parts.
All inputs are finite; a program needn't handle non-finite values.
Results may differ from the reference program's by a relative error of at most 0.00009.
Values sent between devices are 32-bit elements; how exact they have to be, the bound alone decides.
No kernel may reach another device: no remote copies, remote signals or barrier semaphores. Data moves between devices by JAX's collectives and lax.ppermute only.
A program may use at most 64 MiB of HBM per device.

```python
import jax
import jax.numpy as jnp
from jax import lax

G = 2000
K = 64
NCELLS = 65536


def shard_levels(key, dims, cuts, low, top_value):
    level = 1.0
    for dim, shards_of in cuts:
        steps = jax.random.uniform(jax.random.fold_in(jax.random.fold_in(key, 6), dim), (shards_of,), jnp.float32, low / len(cuts), top_value / len(cuts))
        level = level * jnp.repeat(jnp.exp(steps), dims[dim] // shards_of).reshape((-1,) + (1,) * (len(dims) - 1 - dim))
    return level


def scatter_about(stream_key, extent, spread, limit, split=(), kind=jnp.bfloat16):
    loudness = shard_levels(stream_key, extent, split, -0.22, 0.18) if split else 1.0
    entries = jax.random.normal(stream_key, extent, jnp.float32) * spread * loudness
    return jnp.minimum(jnp.maximum(entries, -limit), limit).astype(kind)


def setup_inputs(seed: int = 0, part: int = 0) -> dict:
    key_list = jax.random.split(jax.random.key(seed), 3)
    own_keys = jax.random.split(jax.random.fold_in(key_list[2], part), 3)
    datasets = scatter_about(own_keys[0], (2, G, NCELLS), 1.0, 6.0, ((0, 2), (2, 128)), jnp.float32)
    sketch = scatter_about(own_keys[1], (K, NCELLS), 1.0, 6.0, ((1, 128),), jnp.float32)
    return {"datasets": datasets, "sketch": sketch}


def reference(datasets, sketch):
    high = lax.Precision.HIGHEST
    first = datasets[0]
    second = datasets[1]
    panel = jnp.dot(sketch, second.T, precision=high)
    range_rows = jnp.dot(panel, first, precision=high)
    gram = jnp.dot(range_rows, range_rows.T, precision=high)
    lower = jnp.linalg.cholesky(gram)
    basis = jax.scipy.linalg.solve_triangular(lower, range_rows, lower=True)
    cross = jnp.dot(basis, first.T, precision=high)
    projected = jnp.dot(cross, second, precision=high)
    scale = jnp.sqrt(jnp.float32(NCELLS))
    return jnp.stack([basis * scale, projected / scale])
```

```python
import jax
import jax.numpy as jnp
from jax import lax
from jax.sharding import Mesh
from jax.sharding import PartitionSpec as P

Z_LOW = 4
X_SIZE = 4
GROUPS_CELLS = ("groups", "z_high", "z_low", "x")
NEAR = ("z_low", "x")
FAR = "z_high"
ROWS = 8


def exchanged(blocks, axes):
    return lax.all_to_all(blocks, axes, 0, 0, tiled=True)


def to_all(x, axes):
    return exchanged(jnp.broadcast_to(x[None], (lax.axis_size(axes), *x.shape)), axes)


def sum_over_cells(half):
    rows, cols = half.shape
    part = cols // Z_LOW
    blocks = half.reshape(X_SIZE, ROWS, Z_LOW, part).transpose(2, 0, 1, 3)
    blocks = blocks.reshape(Z_LOW * X_SIZE, ROWS, part)
    own = jnp.sum(exchanged(blocks, NEAR), axis=0)
    own = jnp.sum(to_all(own, FAR), axis=0)
    whole = to_all(own, NEAR).reshape(Z_LOW, X_SIZE, ROWS, part)
    return whole.transpose(1, 2, 0, 3).reshape(rows, cols)


def per_device(datasets, sketch):
    high = lax.Precision.HIGHEST
    own_data = datasets[0]
    genes = own_data.shape[0]
    k = sketch.shape[0]
    half = k // 2
    wide = -(-(genes + 48) // (128 * Z_LOW)) * 128 * Z_LOW
    on_x = lax.axis_index("side") == 0
    cell_count = own_data.shape[1] * lax.axis_size(GROUPS_CELLS[1:])
    scale = jnp.sqrt(jnp.float32(cell_count))

    partial_panel = jnp.dot(sketch, own_data.T, precision=high)
    partial_panel = jnp.pad(partial_panel, ((0, 0), (0, wide - genes)))
    moved = lax.ppermute(partial_panel[:half], "side", [(1, 0)])
    mine = sum_over_cells(jnp.where(on_x, moved, partial_panel[half:]))
    other = lax.ppermute(mine, "side", [(1, 0)])
    panel = jnp.concatenate([mine, other])[:, :genes]

    range_rows = jnp.dot(panel, own_data, precision=high)
    gram = jnp.dot(range_rows, range_rows.T, precision=high)
    corner = gram[half:, half:]
    packed = jnp.concatenate([gram[:, :half], jnp.concatenate([corner[:, : half // 2], corner[:, half // 2 :]])], axis=1)
    raw = jnp.dot(range_rows, own_data.T, precision=high)
    raw = jnp.concatenate([raw, packed, jnp.zeros((k, wide - genes - packed.shape[1]), raw.dtype)], axis=1)
    moved = lax.ppermute(raw[half:], "side", [(0, 1)])
    mine = sum_over_cells(jnp.where(on_x, raw[:half], moved))
    other = lax.ppermute(mine, "side", [(0, 1), (1, 0)])
    total = jnp.concatenate([jnp.where(on_x, mine, other), jnp.where(on_x, other, mine)])

    raw_cross = total[:, :genes]
    packed = total[:, genes : genes + half + half // 2]
    corner = packed[:, half:]
    corner = jnp.concatenate([corner[:half], corner[half:]], axis=1)
    gram = jnp.concatenate([packed[:, :half], jnp.concatenate([jnp.zeros_like(corner), corner])], axis=1)
    lower = lax.linalg.cholesky(gram, symmetrize_input=False)
    inverse = jax.scipy.linalg.solve_triangular(lower, jnp.eye(k, dtype=gram.dtype), lower=True)
    cross = jnp.dot(inverse, raw_cross, precision=high)
    left = jnp.where(on_x, inverse * scale, 0)
    basis = jnp.dot(left, range_rows, precision=high)
    projected = jnp.dot(cross, own_data, precision=high)
    return jnp.where(on_x, basis, projected / scale)[None]


def solution(mesh):
    devices = mesh.devices.reshape(mesh.shape["groups"], -1, Z_LOW, X_SIZE, mesh.shape["side"])
    split = Mesh(devices, (*GROUPS_CELLS, "side"))
    return jax.shard_map(
        per_device,
        mesh=split,
        in_specs=(P("side", None, GROUPS_CELLS), P(None, GROUPS_CELLS)),
        out_specs=P("side", None, GROUPS_CELLS),
        check_vma=False,
    )
```

```python
import functools

import jax
import jax.numpy as jnp
from jax import lax
from jax.experimental import pallas as pl
from jax.experimental.pallas import tpu as pltpu
from jax.sharding import Mesh
from jax.sharding import PartitionSpec as P

Z_LOW = 4
X_SIZE = 4
GROUPS_CELLS = ("groups", "z_high", "z_low", "x")
NEAR = ("z_low", "x")
FAR = "z_high"
ROWS = 8
LANES = 128
STEP = 256
F32 = jnp.float32
BF16 = jnp.bfloat16
HIGH = lax.Precision.HIGHEST
VMEM = pl.BlockSpec(memory_space=pltpu.VMEM)
ANY = pl.BlockSpec(memory_space=pl.ANY)
SMEM = pl.BlockSpec(memory_space=pltpu.SMEM)


def exchanged(blocks, axes):
    return lax.all_to_all(blocks, axes, 0, 0, tiled=True)


def to_all(x, axes):
    return exchanged(jnp.broadcast_to(x[None], (lax.axis_size(axes), *x.shape)), axes)


def sum_over_cells(blocks):
    own = jnp.sum(exchanged(blocks, NEAR), axis=0)
    own = jnp.sum(to_all(own, FAR), axis=0)
    return to_all(own, NEAR)


def halves(x):
    top = x.astype(BF16)
    return top, (x - top.astype(F32)).astype(BF16)


def times(a, b):
    return lax.dot_general(a, b, (((1,), (0,)), ((), ())), preferred_element_type=F32)


def times_t(a, b):
    return lax.dot_general(a, b, (((1,), (1,)), ((), ())), preferred_element_type=F32)


def three(product, stacked, top, low, k):
    both = product(stacked, top)
    return both[:k] + both[k:] + product(stacked[:k], low)


def put_blocks(send_ref, keep_ref, value, first, flip):
    width = value.shape[1]
    part = send_ref.shape[2]
    col = first % part
    half = value.shape[0] // 2
    for x in range(X_SIZE):
        b = first // part * X_SIZE + x
        upper = value[ROWS * x : ROWS * (x + 1)]
        lower = value[half + ROWS * x : half + ROWS * (x + 1)]
        send_ref[b, :, col : col + width] = lower if flip else upper
        keep_ref[b, :, col : col + width] = upper if flip else lower


def whole_rows(block_ref, z):
    return jnp.concatenate([block_ref[z * X_SIZE + x] for x in range(X_SIZE)], axis=0)


def panel_kernel(sketch_ref, data_ref, top_ref, low_ref, send_ref, keep_ref, held, sems):
    genes, cells = held.shape
    wide = top_ref.shape[0]
    k = sketch_ref.shape[0]
    copies = []
    for i, first in enumerate(range(0, genes, STEP)):
        rows = min(STEP, genes - first)
        copy = pltpu.make_async_copy(data_ref.at[0, pl.ds(first, rows)], held.at[pl.ds(first, rows)], sems.at[i])
        copy.start()
        copies.append(copy)
    top_ref[genes:] = jnp.zeros((wide - genes, cells), BF16)
    low_ref[genes:] = jnp.zeros((wide - genes, cells), BF16)
    stacked = jnp.concatenate(halves(sketch_ref[...]), axis=0)
    for i, first in enumerate(range(0, genes, STEP)):
        rows = min(STEP, genes - first)
        copies[i].wait()
        top, low = halves(held[first : first + rows])
        top_ref[first : first + rows] = top
        low_ref[first : first + rows] = low
        value = three(times_t, stacked, top_ref[first : first + STEP], low_ref[first : first + STEP], k)
        put_blocks(send_ref, keep_ref, value, first, False)


def lanes(shape):
    return lax.broadcasted_iota(jnp.int32, shape, 1)


def sublanes(shape):
    return lax.broadcasted_iota(jnp.int32, shape, 0)


def range_kernel(mine_ref, other_ref, top_ref, low_ref, rows_ref, send_ref, keep_ref, panel):
    k = rows_ref.shape[0]
    half = k // 2
    part = send_ref.shape[2]
    wide = top_ref.shape[0]
    for z in range(Z_LOW):
        cols = slice(z * part, (z + 1) * part)
        for i, ref in enumerate((mine_ref, other_ref)):
            top, low = halves(whole_rows(ref, z))
            panel[i * half : (i + 1) * half, cols] = top
            panel[k + i * half : k + (i + 1) * half, cols] = low
    rows = three(times, panel[...], top_ref[...], low_ref[...], k)
    rows_ref[...] = rows
    stacked = jnp.concatenate(halves(rows), axis=0)
    padded = jnp.concatenate([rows, jnp.zeros((LANES - k, rows.shape[1]), F32)], axis=0)
    gram = lax.dot_general(rows, padded, (((1,), (1,)), ((), ())), precision=HIGH, preferred_element_type=F32)
    near = pltpu.roll(gram, LANES - half - half // 2, 1)
    far = pltpu.roll(gram, LANES - k, 1)
    lane, row = lanes(near.shape), sublanes(near.shape)
    far = jnp.concatenate([far[half:], far[half:]], axis=0)
    packed = jnp.where((lane >= LANES - half // 2) & (row < half), far, near)
    for z in range(Z_LOW):
        cols = slice(z * part, (z + 1) * part)
        value = three(times_t, stacked, top_ref[cols], low_ref[cols], k)
        if z < Z_LOW - 1:
            put_blocks(send_ref, keep_ref, value, z * part, True)
        else:
            last = value[:, part - LANES :]
            last = jnp.where(lane >= LANES - half - half // 2, packed, last)
            put_blocks(send_ref, keep_ref, value[:, : part - LANES], z * part, True)
            put_blocks(send_ref, keep_ref, last, wide - LANES, True)


def factor_inverse(packed, k):
    half = k // 2
    lane, row = lanes((k, LANES)), sublanes((k, LANES))
    near = pltpu.roll(packed, half + half // 2, 1)
    far = pltpu.roll(packed, k, 1)
    far = jnp.concatenate([far[:half], far[:half]], axis=0)
    square = jnp.where(lane >= half + half // 2, far, near)
    square = jnp.where((lane < half) | ((lane < k) & (row >= half)), square, 0.0)
    full = jnp.concatenate([square, jnp.zeros((LANES - k, LANES), F32)], axis=0)
    square = jnp.where((lane >= half) & (lane < k) & (row < half), full.T[:k], square)
    work = jnp.where(lane == row + k, 1.0, square)
    pivots = jnp.ones((k, LANES), F32)
    for j in range(k):
        base = j // ROWS * ROWS
        pivot_row = jnp.broadcast_to(work[j : j + 1], (ROWS, LANES))
        pivot = jnp.broadcast_to(pivot_row[:, j : j + 1], (ROWS, LANES))
        scaled = pivot_row / pivot
        pivots = jnp.where(row == j, jnp.concatenate([pivot] * (k // ROWS), axis=0), pivots)
        below = work[base:]
        column = jnp.where(row[base:] > j, jnp.broadcast_to(below[:, j : j + 1], below.shape), 0.0)
        below = below - column * jnp.concatenate([scaled] * ((k - base) // ROWS), axis=0)
        work = below if base == 0 else jnp.concatenate([work[:base], below], axis=0)
    inverse = pltpu.roll(work * lax.rsqrt(pivots), LANES - k, 1)
    return jnp.where(lane < k, inverse, 0.0)


def factor_kernel(scale, side_ref, mine_ref, other_ref, rows_ref, top_ref, low_ref, out_ref, total, stacked):
    k = rows_ref.shape[0]
    half = k // 2
    wide = top_ref.shape[0]
    part = mine_ref.shape[2]
    on_x = side_ref[0] == 0
    for z in range(Z_LOW):
        cols = slice(z * part, (z + 1) * part)
        mine, other = whole_rows(mine_ref, z), whole_rows(other_ref, z)
        total[:half, cols] = jnp.where(on_x, mine, other)
        total[half:, cols] = jnp.where(on_x, other, mine)
    inverse = factor_inverse(total[:, wide - LANES :], k)[:, :k]

    @pl.when(on_x)
    def _():
        out_ref[0] = lax.dot_general(inverse * scale, rows_ref[...], (((1,), (0,)), ((), ())), precision=HIGH, preferred_element_type=F32)

    @pl.when(jnp.logical_not(on_x))
    def _():
        for z in range(Z_LOW):
            cols = slice(z * part, (z + 1) * part)
            cross = lax.dot_general(inverse, total[:, cols], (((1,), (0,)), ((), ())), precision=HIGH, preferred_element_type=F32)
            top, low = halves(cross)
            stacked[:k, cols] = top
            stacked[k:, cols] = low
        out_ref[0] = three(times, stacked[...], top_ref[...], low_ref[...], k) * (1.0 / scale)


def per_device(datasets, sketch):
    _, genes, cells = datasets.shape
    k = sketch.shape[0]
    wide = -(-(genes + k * 3 // 4) // (LANES * Z_LOW)) * LANES * Z_LOW
    near_count = Z_LOW * X_SIZE
    blocks = jax.ShapeDtypeStruct((near_count, ROWS, wide // Z_LOW), F32)
    parts = jax.ShapeDtypeStruct((wide, cells), BF16)
    on_x = lax.axis_index("side") == 0
    scale = float(cells * lax.axis_size(GROUPS_CELLS[1:])) ** 0.5
    count = -(-genes // STEP)

    top, low, send, keep = pl.pallas_call(
        panel_kernel,
        in_specs=[VMEM, ANY],
        out_specs=[VMEM] * 4,
        out_shape=[parts, parts, blocks, blocks],
        scratch_shapes=[pltpu.VMEM((genes, cells), F32), pltpu.SemaphoreType.DMA((count,))],
        name="panel",
    )(sketch, datasets)
    moved = lax.ppermute(send, "side", [(1, 0)])
    mine = sum_over_cells(jnp.where(on_x, moved, keep))
    other = lax.ppermute(mine, "side", [(1, 0)])

    rows, send, keep = pl.pallas_call(
        range_kernel,
        in_specs=[VMEM] * 4,
        out_specs=[VMEM] * 3,
        out_shape=[jax.ShapeDtypeStruct((k, cells), F32), blocks, blocks],
        scratch_shapes=[pltpu.VMEM((2 * k, wide), BF16)],
        name="range_rows",
    )(mine, other, top, low)
    moved = lax.ppermute(send, "side", [(0, 1)])
    mine = sum_over_cells(jnp.where(on_x, keep, moved))
    other = lax.ppermute(mine, "side", [(0, 1), (1, 0)])

    side = lax.axis_index("side").astype(jnp.int32).reshape(1)
    return pl.pallas_call(
        functools.partial(factor_kernel, scale),
        in_specs=[SMEM] + [VMEM] * 5,
        out_specs=VMEM,
        out_shape=jax.ShapeDtypeStruct((1, k, cells), F32),
        scratch_shapes=[pltpu.VMEM((k, wide), F32), pltpu.VMEM((2 * k, wide), BF16)],
        name="factor",
    )(side, mine, other, rows, top, low)


def solution(mesh):
    devices = mesh.devices.reshape(mesh.shape["groups"], -1, Z_LOW, X_SIZE, mesh.shape["side"])
    split = Mesh(devices, (*GROUPS_CELLS, "side"))
    return jax.shard_map(
        per_device,
        mesh=split,
        in_specs=(P("side", None, GROUPS_CELLS), P(None, GROUPS_CELLS)),
        out_specs=P("side", None, GROUPS_CELLS),
        check_vma=False,
    )
```

```python
import functools

import jax
import jax.numpy as jnp
from jax import lax
from jax.experimental import pallas as pl
from jax.experimental.pallas import tpu as pltpu
from jax.sharding import Mesh
from jax.sharding import PartitionSpec as P

Z_LOW = 4
X_SIZE = 4
GROUPS_CELLS = ("groups", "z_high", "z_low", "x")
NEAR = ("z_low", "x")
FAR = "z_high"
ROWS = 8
LANES = 128
STEP = 256
F32 = jnp.float32
BF16 = jnp.bfloat16
HIGH = lax.Precision.HIGHEST
ROOM = pltpu.CompilerParams(vmem_limit_bytes=20 * 1024 * 1024)
VMEM = pl.BlockSpec(memory_space=pltpu.VMEM)
HBM = pl.BlockSpec(memory_space=pltpu.HBM)
SMEM = pl.BlockSpec(memory_space=pltpu.SMEM)


def exchanged(blocks, axes):
    return lax.all_to_all(blocks, axes, 0, 0, tiled=True)


def to_all(x, axes):
    return exchanged(jnp.broadcast_to(x[None], (lax.axis_size(axes), *x.shape)), axes)


def sum_over_cells(blocks):
    own = jnp.sum(exchanged(blocks, NEAR), axis=0)
    own = jnp.sum(to_all(own, FAR), axis=0)
    return to_all(own, NEAR)


def in_hbm(x):
    return pltpu.with_memory_space_constraint(x, pltpu.HBM)


def halves(x):
    top = x.astype(BF16)
    return top, (x - top.astype(F32)).astype(BF16)


def times(a, b):
    return lax.dot_general(a, b, (((1,), (0,)), ((), ())), preferred_element_type=F32)


def times_t(a, b):
    return lax.dot_general(a, b, (((1,), (1,)), ((), ())), preferred_element_type=F32)


def three(product, stacked, top, low, k):
    both = product(stacked, top)
    return both[:k] + both[k:] + product(stacked[:k], low)


def put_blocks(send_ref, keep_ref, value, first, flip):
    width = value.shape[1]
    part = send_ref.shape[2]
    col = first % part
    half = value.shape[0] // 2
    for x in range(X_SIZE):
        b = first // part * X_SIZE + x
        upper = value[ROWS * x : ROWS * (x + 1)]
        lower = value[half + ROWS * x : half + ROWS * (x + 1)]
        send_ref[b, :, col : col + width] = lower if flip else upper
        keep_ref[b, :, col : col + width] = upper if flip else lower


def whole_rows(block_ref, z):
    return jnp.concatenate([block_ref[z * X_SIZE + x] for x in range(X_SIZE)], axis=0)


def panel_kernel(sketch_in, data_ref, top_ref, low_out, send_ref, keep_ref, sketch_ref, held, low_ref, sems):
    first_copy = pltpu.make_async_copy(sketch_in, sketch_ref, sems.at[sems.shape[0] - 1])
    first_copy.start()
    genes, cells = held.shape
    wide = top_ref.shape[0]
    k = sketch_ref.shape[0]
    copies = []
    for i, first in enumerate(range(0, genes, STEP)):
        rows = min(STEP, genes - first)
        copy = pltpu.make_async_copy(data_ref.at[0, pl.ds(first, rows)], held.at[pl.ds(first, rows)], sems.at[i])
        copy.start()
        copies.append(copy)
    top_ref[genes:] = jnp.zeros((wide - genes, cells), BF16)
    low_ref[genes:] = jnp.zeros((wide - genes, cells), BF16)
    first_copy.wait()
    stacked = jnp.concatenate(halves(sketch_ref[...]), axis=0)
    for i, first in enumerate(range(0, genes, STEP)):
        rows = min(STEP, genes - first)
        copies[i].wait()
        top, low = halves(held[first : first + rows])
        top_ref[first : first + rows] = top
        low_ref[first : first + rows] = low
        value = three(times_t, stacked, top_ref[first : first + STEP], low_ref[first : first + STEP], k)
        put_blocks(send_ref, keep_ref, value, first, False)
        copies[i] = pltpu.make_async_copy(low_ref.at[pl.ds(first, STEP)], low_out.at[pl.ds(first, STEP)], sems.at[i])
        copies[i].start()
    for copy in copies:
        copy.wait()


def lanes(shape):
    return lax.broadcasted_iota(jnp.int32, shape, 1)


def sublanes(shape):
    return lax.broadcasted_iota(jnp.int32, shape, 0)


def range_kernel(mine_ref, other_ref, top_ref, low_in, rows_ref, send_ref, keep_ref, panel, low_ref, sem):
    fetch = pltpu.make_async_copy(low_in, low_ref, sem)
    fetch.start()
    k = rows_ref.shape[0]
    half = k // 2
    part = send_ref.shape[2]
    wide = top_ref.shape[0]
    for z in range(Z_LOW):
        cols = slice(z * part, (z + 1) * part)
        for i, ref in enumerate((mine_ref, other_ref)):
            top, low = halves(whole_rows(ref, z))
            panel[i * half : (i + 1) * half, cols] = top
            panel[k + i * half : k + (i + 1) * half, cols] = low
    both = times(panel[...], top_ref[...])
    fetch.wait()
    rows = both[:k] + both[k:] + times(panel[:k], low_ref[...])
    rows_ref[...] = rows
    stacked = jnp.concatenate(halves(rows), axis=0)
    padded = jnp.concatenate([rows, jnp.zeros((LANES - k, rows.shape[1]), F32)], axis=0)
    gram = lax.dot_general(rows, padded, (((1,), (1,)), ((), ())), precision=HIGH, preferred_element_type=F32)
    near = pltpu.roll(gram, LANES - half - half // 2, 1)
    far = pltpu.roll(gram, LANES - k, 1)
    lane, row = lanes(near.shape), sublanes(near.shape)
    far = jnp.concatenate([far[half:], far[half:]], axis=0)
    packed = jnp.where((lane >= LANES - half // 2) & (row < half), far, near)
    for z in range(Z_LOW):
        cols = slice(z * part, (z + 1) * part)
        value = three(times_t, stacked, top_ref[cols], low_ref[cols], k)
        if z < Z_LOW - 1:
            put_blocks(send_ref, keep_ref, value, z * part, True)
        else:
            last = value[:, part - LANES :]
            last = jnp.where(lane >= LANES - half - half // 2, packed, last)
            put_blocks(send_ref, keep_ref, value[:, : part - LANES], z * part, True)
            put_blocks(send_ref, keep_ref, last, wide - LANES, True)


def repeated(x, count):
    return jnp.concatenate([x] * (count // ROWS), axis=0)


def factor_inverse(packed, k):
    half = k // 2
    lane, row = lanes((k, LANES)), sublanes((k, LANES))
    near = pltpu.roll(packed, half + half // 2, 1)
    far = pltpu.roll(packed, k, 1)
    far = jnp.concatenate([far[:half], far[:half]], axis=0)
    square = jnp.where(lane >= half + half // 2, far, near)
    square = jnp.where((lane < half) | ((lane < k) & (row >= half)), square, 0.0)
    full = jnp.concatenate([square, jnp.zeros((LANES - k, LANES), F32)], axis=0)
    square = jnp.where((lane >= half) & (lane < k) & (row < half), full.T[:k], square)
    work = jnp.where(lane == row + k, 1.0, square)
    near_row = sublanes((ROWS, LANES))
    done = []
    for base in range(0, k, ROWS):
        count = k - base
        below = row[:count]
        block = work[:ROWS]
        columns = [jnp.broadcast_to(work[:, base + c : base + c + 1], (count, LANES)) for c in range(ROWS)]
        pivots = jnp.ones((ROWS, LANES), F32)
        factors, pivot_rows = [], []
        for c in range(ROWS):
            pivot = jnp.broadcast_to(columns[c][c : c + 1], (ROWS, LANES))
            pivots = jnp.where(near_row == c, pivot, pivots)
            reciprocal = repeated(1.0 / pivot, count)
            factor = jnp.where(below > c, columns[c] * reciprocal, 0.0)
            pivot_row = jnp.broadcast_to(block[c : c + 1], (ROWS, LANES))
            factors.append(factor)
            pivot_rows.append(pivot_row)
            for d in range(c + 1, ROWS):
                columns[d] = columns[d] - factor * jnp.broadcast_to(columns[d][c : c + 1], (count, LANES))
            block = block - factor[:ROWS] * pivot_row
        done.append(block * lax.rsqrt(pivots))
        if count > ROWS:
            work = work[ROWS:]
            for factor, pivot_row in zip(factors, pivot_rows):
                work = work - factor[ROWS:] * repeated(pivot_row, count - ROWS)
    inverse = pltpu.roll(jnp.concatenate(done, axis=0), LANES - k, 1)
    return jnp.where(lane < k, inverse, 0.0)


def factor_kernel(scale, side_ref, mine_ref, other_ref, rows_ref, top_ref, low_in, out_ref, total, stacked, low_ref, sem):
    fetch = pltpu.make_async_copy(low_in, low_ref, sem)
    fetch.start()
    k = rows_ref.shape[0]
    half = k // 2
    wide = top_ref.shape[0]
    part = mine_ref.shape[2]
    on_x = side_ref[0] == 0
    for z in range(Z_LOW):
        cols = slice(z * part, (z + 1) * part)
        mine, other = whole_rows(mine_ref, z), whole_rows(other_ref, z)
        total[:half, cols] = jnp.where(on_x, mine, other)
        total[half:, cols] = jnp.where(on_x, other, mine)
    inverse = factor_inverse(total[:, wide - LANES :], k)[:, :k]
    fetch.wait()

    @pl.when(on_x)
    def _():
        out_ref[0] = lax.dot_general(inverse * scale, rows_ref[...], (((1,), (0,)), ((), ())), precision=HIGH, preferred_element_type=F32)

    @pl.when(jnp.logical_not(on_x))
    def _():
        for z in range(Z_LOW):
            cols = slice(z * part, (z + 1) * part)
            cross = lax.dot_general(inverse, total[:, cols], (((1,), (0,)), ((), ())), precision=HIGH, preferred_element_type=F32)
            top, low = halves(cross)
            stacked[:k, cols] = top
            stacked[k:, cols] = low
        out_ref[0] = three(times, stacked[...], top_ref[...], low_ref[...], k) * (1.0 / scale)


def per_device(datasets, sketch):
    _, genes, cells = datasets.shape
    k = sketch.shape[0]
    wide = -(-(genes + k * 3 // 4) // (LANES * Z_LOW)) * LANES * Z_LOW
    near_count = Z_LOW * X_SIZE
    blocks = pltpu.VMEM((near_count, ROWS, wide // Z_LOW), F32)
    on_x = lax.axis_index("side") == 0
    scale = float(cells * lax.axis_size(GROUPS_CELLS[1:])) ** 0.5
    count = -(-genes // STEP)

    top, low, send, keep = pl.pallas_call(
        panel_kernel,
        in_specs=[HBM, HBM],
        out_specs=[VMEM, HBM, VMEM, VMEM],
        out_shape=[pltpu.VMEM((wide, cells), BF16), pltpu.HBM((wide, cells), BF16), blocks, blocks],
        scratch_shapes=[
            pltpu.VMEM((k, cells), F32),
            pltpu.VMEM((genes, cells), F32),
            pltpu.VMEM((wide, cells), BF16),
            pltpu.SemaphoreType.DMA((count + 1,)),
        ],
        compiler_params=ROOM,
        name="panel",
    )(in_hbm(sketch), in_hbm(datasets))
    moved = lax.ppermute(send, "side", [(1, 0)])
    mine = sum_over_cells(jnp.where(on_x, moved, keep))
    other = lax.ppermute(mine, "side", [(1, 0)])

    rows, send, keep = pl.pallas_call(
        range_kernel,
        in_specs=[VMEM] * 3 + [HBM],
        out_specs=[VMEM] * 3,
        out_shape=[pltpu.VMEM((k, cells), F32), blocks, blocks],
        scratch_shapes=[pltpu.VMEM((2 * k, wide), BF16), pltpu.VMEM((wide, cells), BF16), pltpu.SemaphoreType.DMA],
        compiler_params=ROOM,
        name="range_rows",
    )(mine, other, top, in_hbm(low))
    moved = lax.ppermute(send, "side", [(0, 1)])
    mine = sum_over_cells(jnp.where(on_x, keep, moved))
    other = lax.ppermute(mine, "side", [(0, 1), (1, 0)])

    side = lax.axis_index("side").astype(jnp.int32).reshape(1)
    return pl.pallas_call(
        functools.partial(factor_kernel, scale),
        in_specs=[SMEM] + [VMEM] * 4 + [HBM],
        out_specs=VMEM,
        out_shape=jax.ShapeDtypeStruct((1, k, cells), F32),
        scratch_shapes=[pltpu.VMEM((k, wide), F32), pltpu.VMEM((2 * k, wide), BF16), pltpu.VMEM((wide, cells), BF16), pltpu.SemaphoreType.DMA],
        compiler_params=ROOM,
        name="factor",
    )(side, mine, other, rows, top, in_hbm(low))


def solution(mesh):
    devices = mesh.devices.reshape(mesh.shape["groups"], -1, Z_LOW, X_SIZE, mesh.shape["side"])
    split = Mesh(devices, (*GROUPS_CELLS, "side"))
    return jax.shard_map(
        per_device,
        mesh=split,
        in_specs=(P("side", None, GROUPS_CELLS), P(None, GROUPS_CELLS)),
        out_specs=P("side", None, GROUPS_CELLS),
        check_vma=False,
    )
```

```python
import functools

import jax
import jax.numpy as jnp
from jax import lax
from jax.experimental import pallas as pl
from jax.experimental.pallas import tpu as pltpu
from jax.sharding import Mesh
from jax.sharding import PartitionSpec as P

Z_LOW = 4
X_SIZE = 4
GROUPS_CELLS = ("groups", "z_high", "z_low", "x")
NEAR = ("z_low", "x")
FAR = "z_high"
ROWS = 8
TALL = 16
LANES = 128
STEP = 256
F32 = jnp.float32
BF16 = jnp.bfloat16
HIGH = lax.Precision.HIGHEST
ROOM = pltpu.CompilerParams(vmem_limit_bytes=20 * 1024 * 1024)
VMEM = pl.BlockSpec(memory_space=pltpu.VMEM)
HBM = pl.BlockSpec(memory_space=pltpu.HBM)
SMEM = pl.BlockSpec(memory_space=pltpu.SMEM)


def exchanged(blocks, axes):
    return lax.all_to_all(blocks, axes, 0, 0, tiled=True)


def to_all(x, axes):
    return exchanged(jnp.broadcast_to(x[None], (lax.axis_size(axes), *x.shape)), axes)


def across(x, source, offset):
    far = lax.axis_size(FAR)
    pairs = [(2 * i + source, 2 * ((i + offset) % far) + 1 - source) for i in range(far)]
    return lax.ppermute(x, (FAR, "side"), pairs)


def sum_over_cells(blocks, on_x, source):
    on_source = on_x if source == 0 else jnp.logical_not(on_x)
    on_target = jnp.logical_not(on_source)
    own = lax.cond(
        on_source,
        lambda v: jnp.sum(exchanged(v, NEAR), axis=0),
        lambda v: jnp.zeros(v.shape[1:], v.dtype),
        blocks,
    )
    far = lax.axis_size(FAR)
    offsets = sorted(range(far), key=lambda o: min(o, far - o))
    own = sum(across(own, source, o) for o in offsets)
    return lax.cond(on_target, lambda v: to_all(v, NEAR), lambda v: jnp.zeros((Z_LOW * X_SIZE, *v.shape), v.dtype), own)


def in_hbm(x):
    return pltpu.with_memory_space_constraint(x, pltpu.HBM)


def halves(x):
    top = x.astype(BF16)
    return top, (x - top.astype(F32)).astype(BF16)


def times(a, b):
    return lax.dot_general(a, b, (((1,), (0,)), ((), ())), preferred_element_type=F32)


def times_t(a, b):
    return lax.dot_general(a, b, (((1,), (1,)), ((), ())), preferred_element_type=F32)


def three(product, stacked, top, low, k):
    both = product(stacked, top)
    return both[:k] + both[k:] + product(stacked[:k], low)


def put_blocks(out_ref, value, first):
    width = value.shape[1]
    part = out_ref.shape[2]
    col = first % part
    for x in range(X_SIZE):
        out_ref[first // part * X_SIZE + x, :, col : col + width] = value[TALL * x : TALL * (x + 1)]


def whole_rows(block_ref, z):
    return jnp.concatenate([block_ref[z * X_SIZE + x] for x in range(X_SIZE)], axis=0)


def panel_kernel(side_ref, sketch_in, data_ref, top_ref, low_out, out_ref, sketch_ref, held, low_ref, sems):
    first_copy = pltpu.make_async_copy(sketch_in, sketch_ref, sems.at[sems.shape[0] - 1])
    first_copy.start()
    genes, cells = held.shape
    wide = top_ref.shape[0]
    k = sketch_ref.shape[0]
    copies = []
    for i, first in enumerate(range(0, genes, STEP)):
        rows = min(STEP, genes - first)
        copy = pltpu.make_async_copy(data_ref.at[0, pl.ds(first, rows)], held.at[pl.ds(first, rows)], sems.at[i])
        copy.start()
        copies.append(copy)
    top_ref[genes:] = jnp.zeros((wide - genes, cells), BF16)
    low_ref[genes:] = jnp.zeros((wide - genes, cells), BF16)
    first_copy.wait()
    stacked = jnp.concatenate(halves(sketch_ref[...]), axis=0)
    for i, first in enumerate(range(0, genes, STEP)):
        rows = min(STEP, genes - first)
        copies[i].wait()
        top, low = halves(held[first : first + rows])
        top_ref[first : first + rows] = top
        low_ref[first : first + rows] = low
        copies[i] = pltpu.make_async_copy(low_ref.at[pl.ds(first, STEP)], low_out.at[pl.ds(first, STEP)], sems.at[i])
        copies[i].start()

        @pl.when(side_ref[0] == 1)
        def _(first=first):
            value = three(times_t, stacked, top_ref[first : first + STEP], low_ref[first : first + STEP], k)
            put_blocks(out_ref, value, first)

    for copy in copies:
        copy.wait()


def lanes(shape):
    return lax.broadcasted_iota(jnp.int32, shape, 1)


def sublanes(shape):
    return lax.broadcasted_iota(jnp.int32, shape, 0)


def range_kernel(side_ref, whole_ref, top_ref, low_in, rows_ref, out_ref, panel, low_ref, sem):
    @pl.when(side_ref[0] == 0)
    def _():
        fetch = pltpu.make_async_copy(low_in, low_ref, sem)
        fetch.start()
        k = rows_ref.shape[0]
        half = k // 2
        part = out_ref.shape[2]
        wide = top_ref.shape[0]
        for z in range(Z_LOW):
            cols = slice(z * part, (z + 1) * part)
            panel[:k, cols], panel[k:, cols] = halves(whole_rows(whole_ref, z))
        both = times(panel[...], top_ref[...])
        fetch.wait()
        rows = both[:k] + both[k:] + times(panel[:k], low_ref[...])
        rows_ref[...] = rows
        stacked = jnp.concatenate(halves(rows), axis=0)
        padded = jnp.concatenate([rows, jnp.zeros((LANES - k, rows.shape[1]), F32)], axis=0)
        gram = lax.dot_general(rows, padded, (((1,), (1,)), ((), ())), precision=HIGH, preferred_element_type=F32)
        near = pltpu.roll(gram, LANES - half - half // 2, 1)
        far = pltpu.roll(gram, LANES - k, 1)
        lane, row = lanes(near.shape), sublanes(near.shape)
        far = jnp.concatenate([far[half:], far[half:]], axis=0)
        packed = jnp.where((lane >= LANES - half // 2) & (row < half), far, near)
        for z in range(Z_LOW):
            cols = slice(z * part, (z + 1) * part)
            value = three(times_t, stacked, top_ref[cols], low_ref[cols], k)
            if z < Z_LOW - 1:
                put_blocks(out_ref, value, z * part)
            else:
                last = value[:, part - LANES :]
                last = jnp.where(lane >= LANES - half - half // 2, packed, last)
                put_blocks(out_ref, value[:, : part - LANES], z * part)
                put_blocks(out_ref, last, wide - LANES)


def repeated(x, count):
    return jnp.concatenate([x] * (count // ROWS), axis=0)


def factor_inverse(packed, k):
    half = k // 2
    lane, row = lanes((k, LANES)), sublanes((k, LANES))
    near = pltpu.roll(packed, half + half // 2, 1)
    far = pltpu.roll(packed, k, 1)
    far = jnp.concatenate([far[:half], far[:half]], axis=0)
    square = jnp.where(lane >= half + half // 2, far, near)
    square = jnp.where((lane < half) | ((lane < k) & (row >= half)), square, 0.0)
    full = jnp.concatenate([square, jnp.zeros((LANES - k, LANES), F32)], axis=0)
    square = jnp.where((lane >= half) & (lane < k) & (row < half), full.T[:k], square)
    work = jnp.where(lane == row + k, 1.0, square)
    near_row = sublanes((ROWS, LANES))
    done = []
    for base in range(0, k, ROWS):
        count = k - base
        below = row[:count]
        block = work[:ROWS]
        columns = [jnp.broadcast_to(work[:, base + c : base + c + 1], (count, LANES)) for c in range(ROWS)]
        pivots = jnp.ones((ROWS, LANES), F32)
        factors, pivot_rows = [], []
        for c in range(ROWS):
            pivot = jnp.broadcast_to(columns[c][c : c + 1], (ROWS, LANES))
            pivots = jnp.where(near_row == c, pivot, pivots)
            reciprocal = repeated(1.0 / pivot, count)
            factor = jnp.where(below > c, columns[c] * reciprocal, 0.0)
            pivot_row = jnp.broadcast_to(block[c : c + 1], (ROWS, LANES))
            factors.append(factor)
            pivot_rows.append(pivot_row)
            for d in range(c + 1, ROWS):
                columns[d] = columns[d] - factor * jnp.broadcast_to(columns[d][c : c + 1], (count, LANES))
            block = block - factor[:ROWS] * pivot_row
        done.append(block * lax.rsqrt(pivots))
        if count > ROWS:
            work = work[ROWS:]
            for factor, pivot_row in zip(factors, pivot_rows):
                work = work - factor[ROWS:] * repeated(pivot_row, count - ROWS)
    inverse = pltpu.roll(jnp.concatenate(done, axis=0), LANES - k, 1)
    return jnp.where(lane < k, inverse, 0.0)


def projection_kernel(scale, side_ref, whole_ref, top_ref, low_in, out_ref, stacked, low_ref, sem):
    @pl.when(side_ref[0] == 1)
    def _():
        fetch = pltpu.make_async_copy(low_in, low_ref, sem)
        fetch.start()
        k = out_ref.shape[1]
        part = whole_ref.shape[2]
        packed = jnp.concatenate([whole_ref[(Z_LOW - 1) * X_SIZE + x, :, part - LANES :] for x in range(X_SIZE)], axis=0)
        inverse = factor_inverse(packed, k)[:, :k]
        for z in range(Z_LOW):
            cols = slice(z * part, (z + 1) * part)
            cross = lax.dot_general(inverse, whole_rows(whole_ref, z), (((1,), (0,)), ((), ())), precision=HIGH, preferred_element_type=F32)
            stacked[:k, cols], stacked[k:, cols] = halves(cross)
        both = times(stacked[...], top_ref[...])
        fetch.wait()
        out_ref[0] = (both[:k] + both[k:] + times(stacked[:k], low_ref[...])) * (1.0 / scale)


def basis_kernel(scale, side_ref, packed_ref, rows_ref, other_ref, out_ref):
    del other_ref

    @pl.when(side_ref[0] == 0)
    def _():
        k = rows_ref.shape[0]
        packed = jnp.concatenate([packed_ref[x] for x in range(X_SIZE)], axis=0)
        inverse = factor_inverse(packed, k)[:, :k] * scale
        out_ref[0] = lax.dot_general(inverse, rows_ref[...], (((1,), (0,)), ((), ())), precision=HIGH, preferred_element_type=F32)


def per_device(datasets, sketch):
    _, genes, cells = datasets.shape
    k = sketch.shape[0]
    wide = -(-(genes + k * 3 // 4) // (LANES * Z_LOW)) * LANES * Z_LOW
    blocks = pltpu.VMEM((Z_LOW * X_SIZE, TALL, wide // Z_LOW), F32)
    side = lax.axis_index("side").astype(jnp.int32).reshape(1)
    on_x = lax.axis_index("side") == 0
    scale = float(cells * lax.axis_size(GROUPS_CELLS[1:])) ** 0.5
    count = -(-genes // STEP)

    top, low, panel = pl.pallas_call(
        panel_kernel,
        in_specs=[SMEM, HBM, HBM],
        out_specs=[VMEM, HBM, VMEM],
        out_shape=[pltpu.VMEM((wide, cells), BF16), pltpu.HBM((wide, cells), BF16), blocks],
        scratch_shapes=[
            pltpu.VMEM((k, cells), F32),
            pltpu.VMEM((genes, cells), F32),
            pltpu.VMEM((wide, cells), BF16),
            pltpu.SemaphoreType.DMA((count + 1,)),
        ],
        compiler_params=ROOM,
        name="panel",
    )(side, in_hbm(sketch), in_hbm(datasets))
    low = in_hbm(low)
    panel = sum_over_cells(panel, on_x, 1)

    rows, raw = pl.pallas_call(
        range_kernel,
        in_specs=[SMEM] + [VMEM] * 2 + [HBM],
        out_specs=[VMEM] * 2,
        out_shape=[pltpu.VMEM((k, cells), F32), blocks],
        scratch_shapes=[pltpu.VMEM((2 * k, wide), BF16), pltpu.VMEM((wide, cells), BF16), pltpu.SemaphoreType.DMA],
        compiler_params=ROOM,
        name="range_rows",
    )(side, panel, top, low)
    raw = sum_over_cells(raw, on_x, 0)

    packed = raw[(Z_LOW - 1) * X_SIZE :, :, raw.shape[2] - LANES :]
    packed = lax.ppermute(packed, "side", [(1, 0)])
    shape = jax.ShapeDtypeStruct((1, k, cells), F32)
    projected = pl.pallas_call(
        functools.partial(projection_kernel, scale),
        in_specs=[SMEM] + [VMEM] * 2 + [HBM],
        out_specs=VMEM,
        out_shape=pltpu.VMEM(shape.shape, F32),
        scratch_shapes=[pltpu.VMEM((2 * k, wide), BF16), pltpu.VMEM((wide, cells), BF16), pltpu.SemaphoreType.DMA],
        compiler_params=ROOM,
        cost_estimate=pl.CostEstimate(flops=10**9, bytes_accessed=10**6, transcendentals=0),
        name="projection",
    )(side, raw, top, low)
    return pl.pallas_call(
        functools.partial(basis_kernel, scale),
        in_specs=[SMEM] + [VMEM] * 3,
        out_specs=VMEM,
        out_shape=shape,
        input_output_aliases={3: 0},
        compiler_params=ROOM,
        name="basis",
    )(side, packed, rows, projected)


def solution(mesh):
    devices = mesh.devices.reshape(mesh.shape["groups"], -1, Z_LOW, X_SIZE, mesh.shape["side"])
    split = Mesh(devices, (*GROUPS_CELLS, "side"))
    return jax.shard_map(
        per_device,
        mesh=split,
        in_specs=(P("side", None, GROUPS_CELLS), P(None, GROUPS_CELLS)),
        out_specs=P("side", None, GROUPS_CELLS),
        check_vma=False,
    )
```

```python
import functools

import jax
import jax.numpy as jnp
from jax import lax
from jax.experimental import pallas as pl
from jax.experimental.pallas import tpu as pltpu
from jax.sharding import Mesh
from jax.sharding import PartitionSpec as P

Z_LOW = 4
X_SIZE = 4
GROUPS_CELLS = ("groups", "z_high", "z_low", "x")
NEAR = ("z_low", "x")
FAR = "z_high"
ROWS = 8
TALL = 16
LANES = 128
STEP = 512
AHEAD = 4
F32 = jnp.float32
BF16 = jnp.bfloat16
HIGH = lax.Precision.HIGHEST
ROOM = pltpu.CompilerParams(vmem_limit_bytes=20 * 1024 * 1024)
VMEM = pl.BlockSpec(memory_space=pltpu.VMEM)
HBM = pl.BlockSpec(memory_space=pltpu.HBM)
SMEM = pl.BlockSpec(memory_space=pltpu.SMEM)


def exchanged(blocks, axes):
    return lax.all_to_all(blocks, axes, 0, 0, tiled=True)


def to_all(x, axes):
    return exchanged(jnp.broadcast_to(x[None], (lax.axis_size(axes), *x.shape)), axes)


def across(x, source, offset):
    far = lax.axis_size(FAR)
    pairs = [(2 * i + source, 2 * ((i + offset) % far) + 1 - source) for i in range(far)]
    return lax.ppermute(x, (FAR, "side"), pairs)


def sum_over_cells(blocks, on_x, source, beside=None):
    on_source = on_x if source == 0 else jnp.logical_not(on_x)
    on_target = jnp.logical_not(on_source)
    own = lax.cond(
        on_source,
        lambda v: jnp.sum(exchanged(v, NEAR), axis=0),
        lambda v: jnp.zeros(v.shape[1:], v.dtype),
        blocks,
    )
    own, beside = lax.optimization_barrier((own, beside))
    far = lax.axis_size(FAR)
    offsets = sorted(range(far), key=lambda o: min(o, far - o))
    own = sum(across(own, source, o) for o in offsets)
    whole = lax.cond(on_target, lambda v: to_all(v, NEAR), lambda v: jnp.zeros((Z_LOW * X_SIZE, *v.shape), v.dtype), own)
    return whole, beside


def in_hbm(x):
    return pltpu.with_memory_space_constraint(x, pltpu.HBM)


def halves(x):
    top = x.astype(BF16)
    return top, (x - top.astype(F32)).astype(BF16)


def times(a, b):
    return lax.dot_general(a, b, (((1,), (0,)), ((), ())), preferred_element_type=F32)


def times_t(a, b):
    return lax.dot_general(a, b, (((1,), (1,)), ((), ())), preferred_element_type=F32)


def three(product, stacked, top, low, k):
    both = product(stacked, top)
    return both[:k] + both[k:] + product(stacked[:k], low)


def put_blocks(out_ref, value, first):
    width = value.shape[1]
    part = out_ref.shape[2]
    col = first % part
    for x in range(X_SIZE):
        out_ref[first // part * X_SIZE + x, :, col : col + width] = value[TALL * x : TALL * (x + 1)]


def whole_rows(block_ref, z):
    return jnp.concatenate([block_ref[z * X_SIZE + x] for x in range(X_SIZE)], axis=0)


def fetches(data_ref, held, sems):
    genes = held.shape[0]
    copies = []
    for i, first in enumerate(range(0, genes, STEP)):
        rows = min(STEP, genes - first)
        copies.append(pltpu.make_async_copy(data_ref.at[0, pl.ds(first, rows)], held.at[pl.ds(first, rows)], sems.at[i]))
    for copy in copies[:AHEAD]:
        copy.start()
    return copies


def arrived(copies, i):
    copies[i].wait()
    if i + AHEAD < len(copies):
        copies[i + AHEAD].start()


def panel_kernel(side_ref, sketch_in, data_ref, out_ref, sketch_ref, held, sems):
    @pl.when(side_ref[0] == 1)
    def _():
        own_copy = pltpu.make_async_copy(sketch_in, sketch_ref, sems.at[sems.shape[0] - 1])
        own_copy.start()
        copies = fetches(data_ref, held, sems)
        own_copy.wait()
        genes = held.shape[0]
        k = sketch_ref.shape[0]
        stacked = jnp.concatenate(halves(sketch_ref[...]), axis=0)
        for i, first in enumerate(range(0, genes, STEP)):
            rows = min(STEP, genes - first)
            arrived(copies, i)
            data = held[first : first + rows]
            if rows < STEP:
                data = jnp.concatenate([data, jnp.zeros((STEP - rows, data.shape[1]), F32)], axis=0)
            put_blocks(out_ref, three(times_t, stacked, *halves(data), k), first)


def split_kernel(data_ref, top_ref, low_out, held, low_ref, sems):
    genes, cells = held.shape
    wide = top_ref.shape[0]
    copies = fetches(data_ref, held, sems)
    top_ref[genes:] = jnp.zeros((wide - genes, cells), BF16)
    low_ref[genes:] = jnp.zeros((wide - genes, cells), BF16)
    for i, first in enumerate(range(0, genes, STEP)):
        rows = min(STEP, genes - first)
        arrived(copies, i)
        top_ref[first : first + rows], low_ref[first : first + rows] = halves(held[first : first + rows])
    writes = []
    for i, first in enumerate(range(0, genes, STEP)):
        writes.append(pltpu.make_async_copy(low_ref.at[pl.ds(first, STEP)], low_out.at[pl.ds(first, STEP)], sems.at[i]))
        writes[i].start()
    for write in writes:
        write.wait()


def lanes(shape):
    return lax.broadcasted_iota(jnp.int32, shape, 1)


def sublanes(shape):
    return lax.broadcasted_iota(jnp.int32, shape, 0)


def low_parts(low_in, low_ref, sems):
    part = low_ref.shape[0] // Z_LOW
    copies = []
    for z in range(Z_LOW):
        spot = pl.ds(z * part, part)
        copies.append(pltpu.make_async_copy(low_in.at[spot], low_ref.at[spot], sems.at[z]))
        copies[z].start()
    return copies


def three_in_parts(stacked, top_ref, low_ref, copies, k):
    both = times(stacked[...], top_ref[...])
    total = both[:k] + both[k:]
    part = low_ref.shape[0] // Z_LOW
    for z, copy in enumerate(copies):
        copy.wait()
        cols = slice(z * part, (z + 1) * part)
        total = total + times(stacked[:k, cols], low_ref[cols])
    return total


def range_kernel(side_ref, whole_ref, top_ref, low_in, rows_ref, out_ref, panel, low_ref, sems):
    @pl.when(side_ref[0] == 0)
    def _():
        copies = low_parts(low_in, low_ref, sems)
        k = rows_ref.shape[0]
        half = k // 2
        part = out_ref.shape[2]
        wide = top_ref.shape[0]
        for z in range(Z_LOW):
            cols = slice(z * part, (z + 1) * part)
            panel[:k, cols], panel[k:, cols] = halves(whole_rows(whole_ref, z))
        rows = three_in_parts(panel, top_ref, low_ref, copies, k)
        rows_ref[...] = rows
        stacked = jnp.concatenate(halves(rows), axis=0)
        padded = jnp.concatenate([rows, jnp.zeros((LANES - k, rows.shape[1]), F32)], axis=0)
        gram = lax.dot_general(rows, padded, (((1,), (1,)), ((), ())), precision=HIGH, preferred_element_type=F32)
        near = pltpu.roll(gram, LANES - half - half // 2, 1)
        far = pltpu.roll(gram, LANES - k, 1)
        lane, row = lanes(near.shape), sublanes(near.shape)
        far = jnp.concatenate([far[half:], far[half:]], axis=0)
        packed = jnp.where((lane >= LANES - half // 2) & (row < half), far, near)
        for z in range(Z_LOW):
            cols = slice(z * part, (z + 1) * part)
            value = three(times_t, stacked, top_ref[cols], low_ref[cols], k)
            if z < Z_LOW - 1:
                put_blocks(out_ref, value, z * part)
            else:
                last = value[:, part - LANES :]
                last = jnp.where(lane >= LANES - half - half // 2, packed, last)
                put_blocks(out_ref, value[:, : part - LANES], z * part)
                put_blocks(out_ref, last, wide - LANES)


def repeated(x, count):
    return jnp.concatenate([x] * (count // ROWS), axis=0)


def factor_inverse(packed, k):
    half = k // 2
    lane, row = lanes((k, LANES)), sublanes((k, LANES))
    near = pltpu.roll(packed, half + half // 2, 1)
    far = pltpu.roll(packed, k, 1)
    far = jnp.concatenate([far[:half], far[:half]], axis=0)
    square = jnp.where(lane >= half + half // 2, far, near)
    square = jnp.where((lane < half) | ((lane < k) & (row >= half)), square, 0.0)
    full = jnp.concatenate([square, jnp.zeros((LANES - k, LANES), F32)], axis=0)
    square = jnp.where((lane >= half) & (lane < k) & (row < half), full.T[:k], square)
    work = jnp.where(lane == row + k, 1.0, square)
    near_row = sublanes((ROWS, LANES))
    done = []
    for base in range(0, k, ROWS):
        count = k - base
        below = row[:count]
        block = work[:ROWS]
        columns = [jnp.broadcast_to(work[:, base + c : base + c + 1], (count, LANES)) for c in range(ROWS)]
        pivots = jnp.ones((ROWS, LANES), F32)
        factors, pivot_rows = [], []
        for c in range(ROWS):
            pivot = jnp.broadcast_to(columns[c][c : c + 1], (ROWS, LANES))
            pivots = jnp.where(near_row == c, pivot, pivots)
            reciprocal = repeated(1.0 / pivot, count)
            factor = jnp.where(below > c, columns[c] * reciprocal, 0.0)
            pivot_row = jnp.broadcast_to(block[c : c + 1], (ROWS, LANES))
            factors.append(factor)
            pivot_rows.append(pivot_row)
            for d in range(c + 1, ROWS):
                columns[d] = columns[d] - factor * jnp.broadcast_to(columns[d][c : c + 1], (count, LANES))
            block = block - factor[:ROWS] * pivot_row
        done.append(block * lax.rsqrt(pivots))
        if count > ROWS:
            work = work[ROWS:]
            for factor, pivot_row in zip(factors, pivot_rows):
                work = work - factor[ROWS:] * repeated(pivot_row, count - ROWS)
    inverse = pltpu.roll(jnp.concatenate(done, axis=0), LANES - k, 1)
    return jnp.where(lane < k, inverse, 0.0)


def projection_kernel(scale, side_ref, whole_ref, top_ref, low_in, out_ref, stacked, low_ref, held, sems):
    @pl.when(side_ref[0] == 1)
    def _():
        copies = low_parts(low_in, low_ref, sems)
        k = held.shape[0]
        part = whole_ref.shape[2]
        packed = jnp.concatenate([whole_ref[(Z_LOW - 1) * X_SIZE + x, :, part - LANES :] for x in range(X_SIZE)], axis=0)
        inverse = factor_inverse(packed, k)[:, :k]
        for z in range(Z_LOW):
            cols = slice(z * part, (z + 1) * part)
            cross = lax.dot_general(inverse, whole_rows(whole_ref, z), (((1,), (0,)), ((), ())), precision=HIGH, preferred_element_type=F32)
            stacked[:k, cols], stacked[k:, cols] = halves(cross)
        held[...] = three_in_parts(stacked, top_ref, low_ref, copies, k) * (1.0 / scale)
        write = pltpu.make_async_copy(held, out_ref.at[0], sems.at[0])
        write.start()
        write.wait()


def basis_kernel(scale, side_ref, packed_ref, rows_ref, other_ref, out_ref, held, sem):
    del other_ref

    @pl.when(side_ref[0] == 0)
    def _():
        k = rows_ref.shape[0]
        packed = jnp.concatenate([packed_ref[x] for x in range(X_SIZE)], axis=0)
        inverse = factor_inverse(packed, k)[:, :k] * scale
        held[...] = lax.dot_general(inverse, rows_ref[...], (((1,), (0,)), ((), ())), precision=HIGH, preferred_element_type=F32)
        write = pltpu.make_async_copy(held, out_ref.at[0], sem)
        write.start()
        write.wait()


def per_device(datasets, sketch):
    _, genes, cells = datasets.shape
    k = sketch.shape[0]
    wide = -(-(genes + k * 3 // 4) // (LANES * Z_LOW)) * LANES * Z_LOW
    blocks = pltpu.VMEM((Z_LOW * X_SIZE, TALL, wide // Z_LOW), F32)
    side = lax.axis_index("side").astype(jnp.int32).reshape(1)
    on_x = lax.axis_index("side") == 0
    scale = float(cells * lax.axis_size(GROUPS_CELLS[1:])) ** 0.5
    count = -(-genes // STEP)

    datasets = in_hbm(datasets)
    panel = pl.pallas_call(
        panel_kernel,
        in_specs=[SMEM, HBM, HBM],
        out_specs=VMEM,
        out_shape=blocks,
        scratch_shapes=[pltpu.VMEM((k, cells), F32), pltpu.VMEM((genes, cells), F32), pltpu.SemaphoreType.DMA((count + 1,))],
        compiler_params=ROOM,
        name="panel",
    )(side, in_hbm(sketch), datasets)
    panel, datasets = sum_over_cells(panel, on_x, 1, datasets)
    top, low = pl.pallas_call(
        split_kernel,
        in_specs=[HBM],
        out_specs=[VMEM, HBM],
        out_shape=[pltpu.VMEM((wide, cells), BF16), pltpu.HBM((wide, cells), BF16)],
        scratch_shapes=[pltpu.VMEM((genes, cells), F32), pltpu.VMEM((wide, cells), BF16), pltpu.SemaphoreType.DMA((count,))],
        compiler_params=ROOM,
        cost_estimate=pl.CostEstimate(flops=10**9, bytes_accessed=10**6, transcendentals=0),
        name="split",
    )(in_hbm(datasets))
    low = in_hbm(low)

    rows, raw = pl.pallas_call(
        range_kernel,
        in_specs=[SMEM] + [VMEM] * 2 + [HBM],
        out_specs=[VMEM] * 2,
        out_shape=[pltpu.VMEM((k, cells), F32), blocks],
        scratch_shapes=[pltpu.VMEM((2 * k, wide), BF16), pltpu.VMEM((wide, cells), BF16), pltpu.SemaphoreType.DMA((Z_LOW,))],
        compiler_params=ROOM,
        name="range_rows",
    )(side, panel, top, low)
    raw, _ = sum_over_cells(raw, on_x, 0)

    packed = raw[(Z_LOW - 1) * X_SIZE :, :, raw.shape[2] - LANES :]
    packed = lax.ppermute(packed, "side", [(1, 0)])
    projected = pl.pallas_call(
        functools.partial(projection_kernel, scale),
        in_specs=[SMEM] + [VMEM] * 2 + [HBM],
        out_specs=HBM,
        out_shape=pltpu.HBM((1, k, cells), F32),
        scratch_shapes=[
            pltpu.VMEM((2 * k, wide), BF16),
            pltpu.VMEM((wide, cells), BF16),
            pltpu.VMEM((k, cells), F32),
            pltpu.SemaphoreType.DMA((Z_LOW,)),
        ],
        compiler_params=ROOM,
        cost_estimate=pl.CostEstimate(flops=10**9, bytes_accessed=10**6, transcendentals=0),
        name="projection",
    )(side, raw, top, low)
    return pl.pallas_call(
        functools.partial(basis_kernel, scale),
        in_specs=[SMEM] + [VMEM] * 2 + [HBM],
        out_specs=HBM,
        out_shape=pltpu.HBM((1, k, cells), F32),
        scratch_shapes=[pltpu.VMEM((k, cells), F32), pltpu.SemaphoreType.DMA],
        input_output_aliases={3: 0},
        compiler_params=ROOM,
        name="basis",
    )(side, packed, rows, in_hbm(projected))


def solution(mesh):
    devices = mesh.devices.reshape(mesh.shape["groups"], -1, Z_LOW, X_SIZE, mesh.shape["side"])
    split = Mesh(devices, (*GROUPS_CELLS, "side"))
    return jax.shard_map(
        per_device,
        mesh=split,
        in_specs=(P("side", None, GROUPS_CELLS), P(None, GROUPS_CELLS)),
        out_specs=P("side", None, GROUPS_CELLS),
        check_vma=False,
    )
```

```python
import functools

import jax
import jax.numpy as jnp
from jax import lax
from jax.experimental import pallas as pl
from jax.experimental.pallas import tpu as pltpu
from jax.sharding import Mesh
from jax.sharding import PartitionSpec as P

Z_LOW = 4
X_SIZE = 4
GROUPS_CELLS = ("groups", "z_high", "z_low", "x")
NEAR = ("z_low", "x")
FAR = "z_high"
ROWS = 8
TALL = 16
LANES = 128
STEP = 512
AHEAD = 4
F32 = jnp.float32
BF16 = jnp.bfloat16
HIGH = lax.Precision.HIGHEST
ROOM = pltpu.CompilerParams(vmem_limit_bytes=20 * 1024 * 1024)
VMEM = pl.BlockSpec(memory_space=pltpu.VMEM)
HBM = pl.BlockSpec(memory_space=pltpu.HBM)
SMEM = pl.BlockSpec(memory_space=pltpu.SMEM)


def exchanged(blocks, axes):
    return lax.all_to_all(blocks, axes, 0, 0, tiled=True)


def to_all(x, axes):
    return exchanged(jnp.broadcast_to(x[None], (lax.axis_size(axes), *x.shape)), axes)


def across(x, source, offset):
    far = lax.axis_size(FAR)
    pairs = [(2 * i + source, 2 * ((i + offset) % far) + 1 - source) for i in range(far)]
    return lax.ppermute(x, (FAR, "side"), pairs)


def sum_over_cells(blocks, on_x, source, beside=None):
    on_source = on_x if source == 0 else jnp.logical_not(on_x)
    on_target = jnp.logical_not(on_source)
    own = lax.cond(
        on_source,
        lambda v: jnp.sum(exchanged(v, NEAR), axis=0),
        lambda v: jnp.zeros(v.shape[1:], v.dtype),
        blocks,
    )
    own, beside = lax.optimization_barrier((own, beside))
    far = lax.axis_size(FAR)
    reach = [min(o, far - o) for o in range(far)]
    offsets = sorted(range(far), key=lambda o: (reach[o] > 0, reach[o] > far // 4, reach[o] == 1, reach[o]))
    own = sum(across(own, source, o) for o in offsets)
    whole = lax.cond(on_target, lambda v: to_all(v, NEAR), lambda v: jnp.zeros((Z_LOW * X_SIZE, *v.shape), v.dtype), own)
    return whole, beside


def in_hbm(x):
    return pltpu.with_memory_space_constraint(x, pltpu.HBM)


def halves(x):
    top = x.astype(BF16)
    return top, (x - top.astype(F32)).astype(BF16)


def times(a, b):
    return lax.dot_general(a, b, (((1,), (0,)), ((), ())), preferred_element_type=F32)


def times_t(a, b):
    return lax.dot_general(a, b, (((1,), (1,)), ((), ())), preferred_element_type=F32)


def three(product, stacked, top, low, k):
    both = product(stacked, top)
    return both[:k] + both[k:] + product(stacked[:k], low)


def put_blocks(out_ref, value, first):
    width = value.shape[1]
    part = out_ref.shape[2]
    col = first % part
    for x in range(X_SIZE):
        out_ref[first // part * X_SIZE + x, :, col : col + width] = value[TALL * x : TALL * (x + 1)]


def whole_rows(block_ref, z):
    return jnp.concatenate([block_ref[z * X_SIZE + x] for x in range(X_SIZE)], axis=0)


def fetches(data_ref, held, sems):
    genes = held.shape[0]
    copies = []
    for i, first in enumerate(range(0, genes, STEP)):
        rows = min(STEP, genes - first)
        copies.append(pltpu.make_async_copy(data_ref.at[0, pl.ds(first, rows)], held.at[pl.ds(first, rows)], sems.at[i]))
    for copy in copies[:AHEAD]:
        copy.start()
    return copies


def arrived(copies, i):
    copies[i].wait()
    if i + AHEAD < len(copies):
        copies[i + AHEAD].start()


def panel_kernel(side_ref, sketch_in, data_ref, out_ref, sketch_ref, held, sems):
    @pl.when(side_ref[0] == 1)
    def _():
        own_copy = pltpu.make_async_copy(sketch_in, sketch_ref, sems.at[sems.shape[0] - 1])
        own_copy.start()
        copies = fetches(data_ref, held, sems)
        own_copy.wait()
        genes = held.shape[0]
        k = sketch_ref.shape[0]
        stacked = jnp.concatenate(halves(sketch_ref[...]), axis=0)
        for i, first in enumerate(range(0, genes, STEP)):
            rows = min(STEP, genes - first)
            arrived(copies, i)
            data = held[first : first + rows]
            if rows < STEP:
                data = jnp.concatenate([data, jnp.zeros((STEP - rows, data.shape[1]), F32)], axis=0)
            put_blocks(out_ref, three(times_t, stacked, *halves(data), k), first)


def split_kernel(data_ref, top_ref, low_out, held, low_ref, sems):
    genes, cells = held.shape
    wide = top_ref.shape[0]
    copies = fetches(data_ref, held, sems)
    top_ref[genes:] = jnp.zeros((wide - genes, cells), BF16)
    low_ref[genes:] = jnp.zeros((wide - genes, cells), BF16)
    for i, first in enumerate(range(0, genes, STEP)):
        rows = min(STEP, genes - first)
        arrived(copies, i)
        top_ref[first : first + rows], low_ref[first : first + rows] = halves(held[first : first + rows])
    writes = []
    for i, first in enumerate(range(0, genes, STEP)):
        writes.append(pltpu.make_async_copy(low_ref.at[pl.ds(first, STEP)], low_out.at[pl.ds(first, STEP)], sems.at[i]))
        writes[i].start()
    for write in writes:
        write.wait()


def lanes(shape):
    return lax.broadcasted_iota(jnp.int32, shape, 1)


def sublanes(shape):
    return lax.broadcasted_iota(jnp.int32, shape, 0)


def low_parts(low_in, low_ref, sems):
    part = low_ref.shape[0] // Z_LOW
    copies = []
    for z in range(Z_LOW):
        spot = pl.ds(z * part, part)
        copies.append(pltpu.make_async_copy(low_in.at[spot], low_ref.at[spot], sems.at[z]))
        copies[z].start()
    return copies


def three_in_parts(stacked, top_ref, low_ref, copies, k):
    both = times(stacked[...], top_ref[...])
    total = both[:k] + both[k:]
    part = low_ref.shape[0] // Z_LOW
    for z, copy in enumerate(copies):
        copy.wait()
        cols = slice(z * part, (z + 1) * part)
        total = total + times(stacked[:k, cols], low_ref[cols])
    return total


def range_kernel(side_ref, whole_ref, top_ref, low_in, rows_ref, out_ref, panel, low_ref, sems):
    @pl.when(side_ref[0] == 0)
    def _():
        copies = low_parts(low_in, low_ref, sems)
        k = rows_ref.shape[0]
        half = k // 2
        part = out_ref.shape[2]
        wide = top_ref.shape[0]
        for z in range(Z_LOW):
            cols = slice(z * part, (z + 1) * part)
            panel[:k, cols], panel[k:, cols] = halves(whole_rows(whole_ref, z))
        rows = three_in_parts(panel, top_ref, low_ref, copies, k)
        rows_ref[...] = rows
        stacked = jnp.concatenate(halves(rows), axis=0)
        padded = jnp.concatenate([rows, jnp.zeros((LANES - k, rows.shape[1]), F32)], axis=0)
        gram = lax.dot_general(rows, padded, (((1,), (1,)), ((), ())), precision=HIGH, preferred_element_type=F32)
        near = pltpu.roll(gram, LANES - half - half // 2, 1)
        far = pltpu.roll(gram, LANES - k, 1)
        lane, row = lanes(near.shape), sublanes(near.shape)
        far = jnp.concatenate([far[half:], far[half:]], axis=0)
        packed = jnp.where((lane >= LANES - half // 2) & (row < half), far, near)
        for z in range(Z_LOW):
            cols = slice(z * part, (z + 1) * part)
            value = three(times_t, stacked, top_ref[cols], low_ref[cols], k)
            if z < Z_LOW - 1:
                put_blocks(out_ref, value, z * part)
            else:
                last = value[:, part - LANES :]
                last = jnp.where(lane >= LANES - half - half // 2, packed, last)
                put_blocks(out_ref, value[:, : part - LANES], z * part)
                put_blocks(out_ref, last, wide - LANES)


def repeated(x, count):
    return jnp.concatenate([x] * (count // ROWS), axis=0)


def factor_inverse(packed, k):
    half = k // 2
    lane, row = lanes((k, LANES)), sublanes((k, LANES))
    near = pltpu.roll(packed, half + half // 2, 1)
    far = pltpu.roll(packed, k, 1)
    far = jnp.concatenate([far[:half], far[:half]], axis=0)
    square = jnp.where(lane >= half + half // 2, far, near)
    square = jnp.where((lane < half) | ((lane < k) & (row >= half)), square, 0.0)
    full = jnp.concatenate([square, jnp.zeros((LANES - k, LANES), F32)], axis=0)
    square = jnp.where((lane >= half) & (lane < k) & (row < half), full.T[:k], square)
    work = jnp.where(lane == row + k, 1.0, square)
    near_row = sublanes((ROWS, LANES))
    done = []
    for base in range(0, k, ROWS):
        count = k - base
        below = row[:count]
        block = work[:ROWS]
        columns = [jnp.broadcast_to(work[:, base + c : base + c + 1], (count, LANES)) for c in range(ROWS)]
        pivots = jnp.ones((ROWS, LANES), F32)
        factors, pivot_rows = [], []
        for c in range(ROWS):
            pivot = jnp.broadcast_to(columns[c][c : c + 1], (ROWS, LANES))
            pivots = jnp.where(near_row == c, pivot, pivots)
            reciprocal = repeated(1.0 / pivot, count)
            factor = jnp.where(below > c, columns[c] * reciprocal, 0.0)
            pivot_row = jnp.broadcast_to(block[c : c + 1], (ROWS, LANES))
            factors.append(factor)
            pivot_rows.append(pivot_row)
            for d in range(c + 1, ROWS):
                columns[d] = columns[d] - factor * jnp.broadcast_to(columns[d][c : c + 1], (count, LANES))
            block = block - factor[:ROWS] * pivot_row
        done.append(block * lax.rsqrt(pivots))
        if count > ROWS:
            work = work[ROWS:]
            for factor, pivot_row in zip(factors, pivot_rows):
                work = work - factor[ROWS:] * repeated(pivot_row, count - ROWS)
    inverse = pltpu.roll(jnp.concatenate(done, axis=0), LANES - k, 1)
    return jnp.where(lane < k, inverse, 0.0)


def projection_kernel(scale, side_ref, whole_ref, top_ref, low_in, out_ref, stacked, low_ref, held, sems):
    @pl.when(side_ref[0] == 1)
    def _():
        copies = low_parts(low_in, low_ref, sems)
        k = held.shape[0]
        part = whole_ref.shape[2]
        packed = jnp.concatenate([whole_ref[(Z_LOW - 1) * X_SIZE + x, :, part - LANES :] for x in range(X_SIZE)], axis=0)
        inverse = factor_inverse(packed, k)[:, :k]
        for z in range(Z_LOW):
            cols = slice(z * part, (z + 1) * part)
            cross = lax.dot_general(inverse, whole_rows(whole_ref, z), (((1,), (0,)), ((), ())), precision=HIGH, preferred_element_type=F32)
            stacked[:k, cols], stacked[k:, cols] = halves(cross)
        held[...] = three_in_parts(stacked, top_ref, low_ref, copies, k) * (1.0 / scale)
        write = pltpu.make_async_copy(held, out_ref.at[0], sems.at[0])
        write.start()
        write.wait()


def basis_kernel(scale, side_ref, packed_ref, rows_ref, other_ref, out_ref, held, sem):
    del other_ref

    @pl.when(side_ref[0] == 0)
    def _():
        k = rows_ref.shape[0]
        packed = jnp.concatenate([packed_ref[x] for x in range(X_SIZE)], axis=0)
        inverse = factor_inverse(packed, k)[:, :k] * scale
        held[...] = lax.dot_general(inverse, rows_ref[...], (((1,), (0,)), ((), ())), precision=HIGH, preferred_element_type=F32)
        write = pltpu.make_async_copy(held, out_ref.at[0], sem)
        write.start()
        write.wait()


def per_device(datasets, sketch):
    _, genes, cells = datasets.shape
    k = sketch.shape[0]
    wide = -(-(genes + k * 3 // 4) // (LANES * Z_LOW)) * LANES * Z_LOW
    blocks = pltpu.VMEM((Z_LOW * X_SIZE, TALL, wide // Z_LOW), F32)
    side = lax.axis_index("side").astype(jnp.int32).reshape(1)
    on_x = lax.axis_index("side") == 0
    scale = float(cells * lax.axis_size(GROUPS_CELLS[1:])) ** 0.5
    count = -(-genes // STEP)

    datasets = in_hbm(datasets)
    panel = pl.pallas_call(
        panel_kernel,
        in_specs=[SMEM, HBM, HBM],
        out_specs=VMEM,
        out_shape=blocks,
        scratch_shapes=[pltpu.VMEM((k, cells), F32), pltpu.VMEM((genes, cells), F32), pltpu.SemaphoreType.DMA((count + 1,))],
        compiler_params=ROOM,
        name="panel",
    )(side, in_hbm(sketch), datasets)
    panel, datasets = sum_over_cells(panel, on_x, 1, datasets)
    top, low = pl.pallas_call(
        split_kernel,
        in_specs=[HBM],
        out_specs=[VMEM, HBM],
        out_shape=[pltpu.VMEM((wide, cells), BF16), pltpu.HBM((wide, cells), BF16)],
        scratch_shapes=[pltpu.VMEM((genes, cells), F32), pltpu.VMEM((wide, cells), BF16), pltpu.SemaphoreType.DMA((count,))],
        compiler_params=ROOM,
        cost_estimate=pl.CostEstimate(flops=10**9, bytes_accessed=10**6, transcendentals=0),
        name="split",
    )(in_hbm(datasets))
    low = in_hbm(low)

    rows, raw = pl.pallas_call(
        range_kernel,
        in_specs=[SMEM] + [VMEM] * 2 + [HBM],
        out_specs=[VMEM] * 2,
        out_shape=[pltpu.VMEM((k, cells), F32), blocks],
        scratch_shapes=[pltpu.VMEM((2 * k, wide), BF16), pltpu.VMEM((wide, cells), BF16), pltpu.SemaphoreType.DMA((Z_LOW,))],
        compiler_params=ROOM,
        name="range_rows",
    )(side, panel, top, low)
    raw, _ = sum_over_cells(raw, on_x, 0)

    packed = raw[(Z_LOW - 1) * X_SIZE :, :, raw.shape[2] - LANES :]
    packed = lax.ppermute(packed, "side", [(1, 0)])
    projected = pl.pallas_call(
        functools.partial(projection_kernel, scale),
        in_specs=[SMEM] + [VMEM] * 2 + [HBM],
        out_specs=HBM,
        out_shape=pltpu.HBM((1, k, cells), F32),
        scratch_shapes=[
            pltpu.VMEM((2 * k, wide), BF16),
            pltpu.VMEM((wide, cells), BF16),
            pltpu.VMEM((k, cells), F32),
            pltpu.SemaphoreType.DMA((Z_LOW,)),
        ],
        compiler_params=ROOM,
        cost_estimate=pl.CostEstimate(flops=10**9, bytes_accessed=10**6, transcendentals=0),
        name="projection",
    )(side, raw, top, low)
    return pl.pallas_call(
        functools.partial(basis_kernel, scale),
        in_specs=[SMEM] + [VMEM] * 2 + [HBM],
        out_specs=HBM,
        out_shape=pltpu.HBM((1, k, cells), F32),
        scratch_shapes=[pltpu.VMEM((k, cells), F32), pltpu.SemaphoreType.DMA],
        input_output_aliases={3: 0},
        compiler_params=ROOM,
        name="basis",
    )(side, packed, rows, in_hbm(projected))


def solution(mesh):
    devices = mesh.devices.reshape(mesh.shape["groups"], -1, Z_LOW, X_SIZE, mesh.shape["side"])
    split = Mesh(devices, (*GROUPS_CELLS, "side"))
    return jax.shard_map(
        per_device,
        mesh=split,
        in_specs=(P("side", None, GROUPS_CELLS), P(None, GROUPS_CELLS)),
        out_specs=P("side", None, GROUPS_CELLS),
        check_vma=False,
    )
```

```python
import functools

import jax
import jax.numpy as jnp
from jax import lax
from jax.experimental import pallas as pl
from jax.experimental.pallas import tpu as pltpu
from jax.sharding import Mesh
from jax.sharding import PartitionSpec as P

Z_LOW = 4
X_SIZE = 4
GROUPS_CELLS = ("groups", "z_high", "z_low", "x")
NEAR = ("z_low", "x")
FAR = "z_high"
ROWS = 8
TALL = 16
LANES = 128
STEP = 512
AHEAD = 4
F32 = jnp.float32
BF16 = jnp.bfloat16
HIGH = lax.Precision.HIGHEST
ROOM = pltpu.CompilerParams(vmem_limit_bytes=20 * 1024 * 1024)
VMEM = pl.BlockSpec(memory_space=pltpu.VMEM)
HBM = pl.BlockSpec(memory_space=pltpu.HBM)
SMEM = pl.BlockSpec(memory_space=pltpu.SMEM)


def exchanged(blocks, axes):
    return lax.all_to_all(blocks, axes, 0, 0, tiled=True)


def to_all(x, axes):
    return exchanged(jnp.broadcast_to(x[None], (lax.axis_size(axes), *x.shape)), axes)


def across(x, source, offset):
    far = lax.axis_size(FAR)
    pairs = [(2 * i + source, 2 * ((i + offset) % far) + 1 - source) for i in range(far)]
    return lax.ppermute(x, (FAR, "side"), pairs)


def sum_over_cells(blocks, on_x, source, beside=None):
    on_source = on_x if source == 0 else jnp.logical_not(on_x)
    on_target = jnp.logical_not(on_source)
    own = lax.cond(
        on_source,
        lambda v: jnp.sum(exchanged(v, NEAR), axis=0),
        lambda v: jnp.zeros(v.shape[1:], v.dtype),
        blocks,
    )
    own, beside = lax.optimization_barrier((own, beside))
    far = lax.axis_size(FAR)
    reach = [min(o, far - o) for o in range(far)]
    offsets = sorted(range(far), key=lambda o: reach[o] or 1.5)
    own = sum(across(own, source, o) for o in offsets)
    whole = lax.cond(on_target, lambda v: to_all(v, NEAR), lambda v: jnp.zeros((Z_LOW * X_SIZE, *v.shape), v.dtype), own)
    return whole, beside


def in_hbm(x):
    return pltpu.with_memory_space_constraint(x, pltpu.HBM)


def halves(x):
    top = x.astype(BF16)
    return top, (x - top.astype(F32)).astype(BF16)


def times(a, b):
    return lax.dot_general(a, b, (((1,), (0,)), ((), ())), preferred_element_type=F32)


def times_t(a, b):
    return lax.dot_general(a, b, (((1,), (1,)), ((), ())), preferred_element_type=F32)


def three(product, stacked, top, low, k):
    both = product(stacked, top)
    return both[:k] + both[k:] + product(stacked[:k], low)


def put_blocks(out_ref, value, first):
    width = value.shape[1]
    part = out_ref.shape[2]
    col = first % part
    for x in range(X_SIZE):
        out_ref[first // part * X_SIZE + x, :, col : col + width] = value[TALL * x : TALL * (x + 1)]


def whole_rows(block_ref, z):
    return jnp.concatenate([block_ref[z * X_SIZE + x] for x in range(X_SIZE)], axis=0)


def fetches(data_ref, held, sems):
    genes = held.shape[0]
    copies = []
    for i, first in enumerate(range(0, genes, STEP)):
        rows = min(STEP, genes - first)
        copies.append(pltpu.make_async_copy(data_ref.at[0, pl.ds(first, rows)], held.at[pl.ds(first, rows)], sems.at[i]))
    for copy in copies[:AHEAD]:
        copy.start()
    return copies


def arrived(copies, i):
    copies[i].wait()
    if i + AHEAD < len(copies):
        copies[i + AHEAD].start()


def panel_kernel(side_ref, sketch_in, data_ref, out_ref, sketch_ref, held, sems):
    @pl.when(side_ref[0] == 1)
    def _():
        own_copy = pltpu.make_async_copy(sketch_in, sketch_ref, sems.at[sems.shape[0] - 1])
        own_copy.start()
        copies = fetches(data_ref, held, sems)
        own_copy.wait()
        genes = held.shape[0]
        k = sketch_ref.shape[0]
        stacked = jnp.concatenate(halves(sketch_ref[...]), axis=0)
        for i, first in enumerate(range(0, genes, STEP)):
            rows = min(STEP, genes - first)
            arrived(copies, i)
            data = held[first : first + rows]
            if rows < STEP:
                data = jnp.concatenate([data, jnp.zeros((STEP - rows, data.shape[1]), F32)], axis=0)
            put_blocks(out_ref, three(times_t, stacked, *halves(data), k), first)


def split_kernel(data_ref, top_ref, low_out, held, low_ref, sems):
    genes, cells = held.shape
    wide = top_ref.shape[0]
    copies = fetches(data_ref, held, sems)
    top_ref[genes:] = jnp.zeros((wide - genes, cells), BF16)
    low_ref[genes:] = jnp.zeros((wide - genes, cells), BF16)
    for i, first in enumerate(range(0, genes, STEP)):
        rows = min(STEP, genes - first)
        arrived(copies, i)
        top_ref[first : first + rows], low_ref[first : first + rows] = halves(held[first : first + rows])
    writes = []
    for i, first in enumerate(range(0, genes, STEP)):
        writes.append(pltpu.make_async_copy(low_ref.at[pl.ds(first, STEP)], low_out.at[pl.ds(first, STEP)], sems.at[i]))
        writes[i].start()
    for write in writes:
        write.wait()


def lanes(shape):
    return lax.broadcasted_iota(jnp.int32, shape, 1)


def sublanes(shape):
    return lax.broadcasted_iota(jnp.int32, shape, 0)


def low_parts(low_in, low_ref, sems):
    part = low_ref.shape[0] // Z_LOW
    copies = []
    for z in range(Z_LOW):
        spot = pl.ds(z * part, part)
        copies.append(pltpu.make_async_copy(low_in.at[spot], low_ref.at[spot], sems.at[z]))
        copies[z].start()
    return copies


def three_in_parts(stacked, top_ref, low_ref, copies, k):
    both = times(stacked[...], top_ref[...])
    total = both[:k] + both[k:]
    part = low_ref.shape[0] // Z_LOW
    for z, copy in enumerate(copies):
        copy.wait()
        cols = slice(z * part, (z + 1) * part)
        total = total + times(stacked[:k, cols], low_ref[cols])
    return total


def range_kernel(side_ref, whole_ref, top_ref, low_in, rows_ref, out_ref, panel, low_ref, sems):
    @pl.when(side_ref[0] == 0)
    def _():
        copies = low_parts(low_in, low_ref, sems)
        k = rows_ref.shape[0]
        half = k // 2
        part = out_ref.shape[2]
        wide = top_ref.shape[0]
        for z in range(Z_LOW):
            cols = slice(z * part, (z + 1) * part)
            panel[:k, cols], panel[k:, cols] = halves(whole_rows(whole_ref, z))
        rows = three_in_parts(panel, top_ref, low_ref, copies, k)
        rows_ref[...] = rows
        stacked = jnp.concatenate(halves(rows), axis=0)
        padded = jnp.concatenate([rows, jnp.zeros((LANES - k, rows.shape[1]), F32)], axis=0)
        gram = lax.dot_general(rows, padded, (((1,), (1,)), ((), ())), precision=HIGH, preferred_element_type=F32)
        near = pltpu.roll(gram, LANES - half - half // 2, 1)
        far = pltpu.roll(gram, LANES - k, 1)
        lane, row = lanes(near.shape), sublanes(near.shape)
        far = jnp.concatenate([far[half:], far[half:]], axis=0)
        packed = jnp.where((lane >= LANES - half // 2) & (row < half), far, near)
        for z in range(Z_LOW):
            cols = slice(z * part, (z + 1) * part)
            value = three(times_t, stacked, top_ref[cols], low_ref[cols], k)
            if z < Z_LOW - 1:
                put_blocks(out_ref, value, z * part)
            else:
                last = value[:, part - LANES :]
                last = jnp.where(lane >= LANES - half - half // 2, packed, last)
                put_blocks(out_ref, value[:, : part - LANES], z * part)
                put_blocks(out_ref, last, wide - LANES)


def repeated(x, count):
    return jnp.concatenate([x] * (count // ROWS), axis=0)


def factor_inverse(packed, k):
    half = k // 2
    lane, row = lanes((k, LANES)), sublanes((k, LANES))
    near = pltpu.roll(packed, half + half // 2, 1)
    far = pltpu.roll(packed, k, 1)
    far = jnp.concatenate([far[:half], far[:half]], axis=0)
    square = jnp.where(lane >= half + half // 2, far, near)
    square = jnp.where((lane < half) | ((lane < k) & (row >= half)), square, 0.0)
    full = jnp.concatenate([square, jnp.zeros((LANES - k, LANES), F32)], axis=0)
    square = jnp.where((lane >= half) & (lane < k) & (row < half), full.T[:k], square)
    work = jnp.where(lane == row + k, 1.0, square)
    near_row = sublanes((ROWS, LANES))
    done = []
    for base in range(0, k, ROWS):
        count = k - base
        below = row[:count]
        block = work[:ROWS]
        columns = [jnp.broadcast_to(work[:, base + c : base + c + 1], (count, LANES)) for c in range(ROWS)]
        pivots = jnp.ones((ROWS, LANES), F32)
        factors, pivot_rows = [], []
        for c in range(ROWS):
            pivot = jnp.broadcast_to(columns[c][c : c + 1], (ROWS, LANES))
            pivots = jnp.where(near_row == c, pivot, pivots)
            reciprocal = repeated(1.0 / pivot, count)
            factor = jnp.where(below > c, columns[c] * reciprocal, 0.0)
            pivot_row = jnp.broadcast_to(block[c : c + 1], (ROWS, LANES))
            factors.append(factor)
            pivot_rows.append(pivot_row)
            for d in range(c + 1, ROWS):
                columns[d] = columns[d] - factor * jnp.broadcast_to(columns[d][c : c + 1], (count, LANES))
            block = block - factor[:ROWS] * pivot_row
        done.append(block * lax.rsqrt(pivots))
        if count > ROWS:
            work = work[ROWS:]
            for factor, pivot_row in zip(factors, pivot_rows):
                work = work - factor[ROWS:] * repeated(pivot_row, count - ROWS)
    inverse = pltpu.roll(jnp.concatenate(done, axis=0), LANES - k, 1)
    return jnp.where(lane < k, inverse, 0.0)


def projection_kernel(scale, side_ref, whole_ref, top_ref, low_in, out_ref, stacked, low_ref, held, sems):
    @pl.when(side_ref[0] == 1)
    def _():
        copies = low_parts(low_in, low_ref, sems)
        k = held.shape[0]
        part = whole_ref.shape[2]
        packed = jnp.concatenate([whole_ref[(Z_LOW - 1) * X_SIZE + x, :, part - LANES :] for x in range(X_SIZE)], axis=0)
        inverse = factor_inverse(packed, k)[:, :k]
        for z in range(Z_LOW):
            cols = slice(z * part, (z + 1) * part)
            cross = lax.dot_general(inverse, whole_rows(whole_ref, z), (((1,), (0,)), ((), ())), precision=HIGH, preferred_element_type=F32)
            stacked[:k, cols], stacked[k:, cols] = halves(cross)
        held[...] = three_in_parts(stacked, top_ref, low_ref, copies, k) * (1.0 / scale)
        write = pltpu.make_async_copy(held, out_ref.at[0], sems.at[0])
        write.start()
        write.wait()


def basis_kernel(scale, side_ref, packed_ref, rows_ref, other_ref, out_ref, held, sem):
    del other_ref

    @pl.when(side_ref[0] == 0)
    def _():
        k = rows_ref.shape[0]
        packed = jnp.concatenate([packed_ref[x] for x in range(X_SIZE)], axis=0)
        inverse = factor_inverse(packed, k)[:, :k] * scale
        held[...] = lax.dot_general(inverse, rows_ref[...], (((1,), (0,)), ((), ())), precision=HIGH, preferred_element_type=F32)
        write = pltpu.make_async_copy(held, out_ref.at[0], sem)
        write.start()
        write.wait()


def per_device(datasets, sketch):
    _, genes, cells = datasets.shape
    k = sketch.shape[0]
    wide = -(-(genes + k * 3 // 4) // (LANES * Z_LOW)) * LANES * Z_LOW
    blocks = pltpu.VMEM((Z_LOW * X_SIZE, TALL, wide // Z_LOW), F32)
    side = lax.axis_index("side").astype(jnp.int32).reshape(1)
    on_x = lax.axis_index("side") == 0
    scale = float(cells * lax.axis_size(GROUPS_CELLS[1:])) ** 0.5
    count = -(-genes // STEP)

    datasets = in_hbm(datasets)
    panel = pl.pallas_call(
        panel_kernel,
        in_specs=[SMEM, HBM, HBM],
        out_specs=VMEM,
        out_shape=blocks,
        scratch_shapes=[pltpu.VMEM((k, cells), F32), pltpu.VMEM((genes, cells), F32), pltpu.SemaphoreType.DMA((count + 1,))],
        compiler_params=ROOM,
        name="panel",
    )(side, in_hbm(sketch), datasets)
    panel, datasets = sum_over_cells(panel, on_x, 1, datasets)
    top, low = pl.pallas_call(
        split_kernel,
        in_specs=[HBM],
        out_specs=[VMEM, HBM],
        out_shape=[pltpu.VMEM((wide, cells), BF16), pltpu.HBM((wide, cells), BF16)],
        scratch_shapes=[pltpu.VMEM((genes, cells), F32), pltpu.VMEM((wide, cells), BF16), pltpu.SemaphoreType.DMA((count,))],
        compiler_params=ROOM,
        cost_estimate=pl.CostEstimate(flops=10**9, bytes_accessed=10**6, transcendentals=0),
        name="split",
    )(in_hbm(datasets))
    low = in_hbm(low)

    rows, raw = pl.pallas_call(
        range_kernel,
        in_specs=[SMEM] + [VMEM] * 2 + [HBM],
        out_specs=[VMEM] * 2,
        out_shape=[pltpu.VMEM((k, cells), F32), blocks],
        scratch_shapes=[pltpu.VMEM((2 * k, wide), BF16), pltpu.VMEM((wide, cells), BF16), pltpu.SemaphoreType.DMA((Z_LOW,))],
        compiler_params=ROOM,
        name="range_rows",
    )(side, panel, top, low)
    raw, _ = sum_over_cells(raw, on_x, 0)

    packed = raw[(Z_LOW - 1) * X_SIZE :, :, raw.shape[2] - LANES :]
    packed = lax.ppermute(packed, "side", [(1, 0)])
    projected = pl.pallas_call(
        functools.partial(projection_kernel, scale),
        in_specs=[SMEM] + [VMEM] * 2 + [HBM],
        out_specs=HBM,
        out_shape=pltpu.HBM((1, k, cells), F32),
        scratch_shapes=[
            pltpu.VMEM((2 * k, wide), BF16),
            pltpu.VMEM((wide, cells), BF16),
            pltpu.VMEM((k, cells), F32),
            pltpu.SemaphoreType.DMA((Z_LOW,)),
        ],
        compiler_params=ROOM,
        cost_estimate=pl.CostEstimate(flops=10**9, bytes_accessed=10**6, transcendentals=0),
        name="projection",
    )(side, raw, top, low)
    return pl.pallas_call(
        functools.partial(basis_kernel, scale),
        in_specs=[SMEM] + [VMEM] * 2 + [HBM],
        out_specs=HBM,
        out_shape=pltpu.HBM((1, k, cells), F32),
        scratch_shapes=[pltpu.VMEM((k, cells), F32), pltpu.SemaphoreType.DMA],
        input_output_aliases={3: 0},
        compiler_params=ROOM,
        name="basis",
    )(side, packed, rows, in_hbm(projected))


def solution(mesh):
    devices = mesh.devices.reshape(mesh.shape["groups"], -1, Z_LOW, X_SIZE, mesh.shape["side"])
    split = Mesh(devices, (*GROUPS_CELLS, "side"))
    return jax.shard_map(
        per_device,
        mesh=split,
        in_specs=(P("side", None, GROUPS_CELLS), P(None, GROUPS_CELLS)),
        out_specs=P("side", None, GROUPS_CELLS),
        check_vma=False,
    )
```

```python
import functools

import jax
import jax.numpy as jnp
from jax import lax
from jax.experimental import pallas as pl
from jax.experimental.pallas import tpu as pltpu
from jax.sharding import Mesh
from jax.sharding import PartitionSpec as P

Z_LOW = 4
X_SIZE = 4
GROUPS_CELLS = ("groups", "z_high", "z_low", "x")
NEAR = ("z_low", "x")
FAR = "z_high"
ROWS = 8
TALL = 16
LANES = 128
STEP = 512
AHEAD = 4
F32 = jnp.float32
BF16 = jnp.bfloat16
HIGH = lax.Precision.HIGHEST
ROOM = pltpu.CompilerParams(vmem_limit_bytes=20 * 1024 * 1024)
VMEM = pl.BlockSpec(memory_space=pltpu.VMEM)
HBM = pl.BlockSpec(memory_space=pltpu.HBM)
SMEM = pl.BlockSpec(memory_space=pltpu.SMEM)


def exchanged(blocks, axes):
    return lax.all_to_all(blocks, axes, 0, 0, tiled=True)


def to_all(x, axes):
    return exchanged(jnp.broadcast_to(x[None], (lax.axis_size(axes), *x.shape)), axes)


def across(x, source, offset):
    far = lax.axis_size(FAR)
    pairs = [(2 * i + source, 2 * ((i + offset) % far) + 1 - source) for i in range(far)]
    return lax.ppermute(x, (FAR, "side"), pairs)


def sum_over_cells(blocks, on_x, source, beside=None):
    on_source = on_x if source == 0 else jnp.logical_not(on_x)
    on_target = jnp.logical_not(on_source)
    own = lax.cond(
        on_source,
        lambda v: jnp.sum(exchanged(v, NEAR), axis=0),
        lambda v: jnp.zeros(v.shape[1:], v.dtype),
        blocks,
    )
    own, beside = lax.optimization_barrier((own, beside))
    far = lax.axis_size(FAR)
    reach = [min(o, far - o) for o in range(far)]
    offsets = sorted(range(far), key=lambda o: (reach[o] > far // 4, reach[o] == 0, reach[o] == 1, reach[o]))
    own = sum(across(own, source, o) for o in offsets)
    whole = lax.cond(on_target, lambda v: to_all(v, NEAR), lambda v: jnp.zeros((Z_LOW * X_SIZE, *v.shape), v.dtype), own)
    return whole, beside


def in_hbm(x):
    return pltpu.with_memory_space_constraint(x, pltpu.HBM)


def halves(x):
    top = x.astype(BF16)
    return top, (x - top.astype(F32)).astype(BF16)


def times(a, b):
    return lax.dot_general(a, b, (((1,), (0,)), ((), ())), preferred_element_type=F32)


def times_t(a, b):
    return lax.dot_general(a, b, (((1,), (1,)), ((), ())), preferred_element_type=F32)


def three(product, stacked, top, low, k):
    both = product(stacked, top)
    return both[:k] + both[k:] + product(stacked[:k], low)


def put_blocks(out_ref, value, first):
    width = value.shape[1]
    part = out_ref.shape[2]
    col = first % part
    for x in range(X_SIZE):
        out_ref[first // part * X_SIZE + x, :, col : col + width] = value[TALL * x : TALL * (x + 1)]


def whole_rows(block_ref, z):
    return jnp.concatenate([block_ref[z * X_SIZE + x] for x in range(X_SIZE)], axis=0)


def fetches(data_ref, held, sems):
    genes = held.shape[0]
    copies = []
    for i, first in enumerate(range(0, genes, STEP)):
        rows = min(STEP, genes - first)
        copies.append(pltpu.make_async_copy(data_ref.at[0, pl.ds(first, rows)], held.at[pl.ds(first, rows)], sems.at[i]))
    for copy in copies[:AHEAD]:
        copy.start()
    return copies


def arrived(copies, i):
    copies[i].wait()
    if i + AHEAD < len(copies):
        copies[i + AHEAD].start()


def panel_kernel(side_ref, sketch_in, data_ref, out_ref, sketch_ref, held, sems):
    @pl.when(side_ref[0] == 1)
    def _():
        own_copy = pltpu.make_async_copy(sketch_in, sketch_ref, sems.at[sems.shape[0] - 1])
        own_copy.start()
        copies = fetches(data_ref, held, sems)
        own_copy.wait()
        genes = held.shape[0]
        k = sketch_ref.shape[0]
        stacked = jnp.concatenate(halves(sketch_ref[...]), axis=0)
        for i, first in enumerate(range(0, genes, STEP)):
            rows = min(STEP, genes - first)
            arrived(copies, i)
            data = held[first : first + rows]
            if rows < STEP:
                data = jnp.concatenate([data, jnp.zeros((STEP - rows, data.shape[1]), F32)], axis=0)
            put_blocks(out_ref, three(times_t, stacked, *halves(data), k), first)


def split_kernel(data_ref, top_ref, low_out, held, low_ref, sems):
    genes, cells = held.shape
    wide = top_ref.shape[0]
    copies = fetches(data_ref, held, sems)
    top_ref[genes:] = jnp.zeros((wide - genes, cells), BF16)
    low_ref[genes:] = jnp.zeros((wide - genes, cells), BF16)
    for i, first in enumerate(range(0, genes, STEP)):
        rows = min(STEP, genes - first)
        arrived(copies, i)
        top_ref[first : first + rows], low_ref[first : first + rows] = halves(held[first : first + rows])
    writes = []
    for i, first in enumerate(range(0, genes, STEP)):
        writes.append(pltpu.make_async_copy(low_ref.at[pl.ds(first, STEP)], low_out.at[pl.ds(first, STEP)], sems.at[i]))
        writes[i].start()
    for write in writes:
        write.wait()


def lanes(shape):
    return lax.broadcasted_iota(jnp.int32, shape, 1)


def sublanes(shape):
    return lax.broadcasted_iota(jnp.int32, shape, 0)


def low_parts(low_in, low_ref, sems):
    part = low_ref.shape[0] // Z_LOW
    copies = []
    for z in range(Z_LOW):
        spot = pl.ds(z * part, part)
        copies.append(pltpu.make_async_copy(low_in.at[spot], low_ref.at[spot], sems.at[z]))
        copies[z].start()
    return copies


def three_in_parts(stacked, top_ref, low_ref, copies, k):
    both = times(stacked[...], top_ref[...])
    total = both[:k] + both[k:]
    part = low_ref.shape[0] // Z_LOW
    for z, copy in enumerate(copies):
        copy.wait()
        cols = slice(z * part, (z + 1) * part)
        total = total + times(stacked[:k, cols], low_ref[cols])
    return total


def range_kernel(side_ref, whole_ref, top_ref, low_in, rows_ref, out_ref, panel, low_ref, sems):
    @pl.when(side_ref[0] == 0)
    def _():
        copies = low_parts(low_in, low_ref, sems)
        k = rows_ref.shape[0]
        half = k // 2
        part = out_ref.shape[2]
        wide = top_ref.shape[0]
        for z in range(Z_LOW):
            cols = slice(z * part, (z + 1) * part)
            panel[:k, cols], panel[k:, cols] = halves(whole_rows(whole_ref, z))
        rows = three_in_parts(panel, top_ref, low_ref, copies, k)
        rows_ref[...] = rows
        stacked = jnp.concatenate(halves(rows), axis=0)
        padded = jnp.concatenate([rows, jnp.zeros((LANES - k, rows.shape[1]), F32)], axis=0)
        gram = lax.dot_general(rows, padded, (((1,), (1,)), ((), ())), precision=HIGH, preferred_element_type=F32)
        near = pltpu.roll(gram, LANES - half - half // 2, 1)
        far = pltpu.roll(gram, LANES - k, 1)
        lane, row = lanes(near.shape), sublanes(near.shape)
        far = jnp.concatenate([far[half:], far[half:]], axis=0)
        packed = jnp.where((lane >= LANES - half // 2) & (row < half), far, near)
        for z in range(Z_LOW):
            cols = slice(z * part, (z + 1) * part)
            value = three(times_t, stacked, top_ref[cols], low_ref[cols], k)
            if z < Z_LOW - 1:
                put_blocks(out_ref, value, z * part)
            else:
                last = value[:, part - LANES :]
                last = jnp.where(lane >= LANES - half - half // 2, packed, last)
                put_blocks(out_ref, value[:, : part - LANES], z * part)
                put_blocks(out_ref, last, wide - LANES)


def repeated(x, count):
    return jnp.concatenate([x] * (count // ROWS), axis=0)


def factor_inverse(packed, k):
    half = k // 2
    lane, row = lanes((k, LANES)), sublanes((k, LANES))
    near = pltpu.roll(packed, half + half // 2, 1)
    far = pltpu.roll(packed, k, 1)
    far = jnp.concatenate([far[:half], far[:half]], axis=0)
    square = jnp.where(lane >= half + half // 2, far, near)
    square = jnp.where((lane < half) | ((lane < k) & (row >= half)), square, 0.0)
    full = jnp.concatenate([square, jnp.zeros((LANES - k, LANES), F32)], axis=0)
    square = jnp.where((lane >= half) & (lane < k) & (row < half), full.T[:k], square)
    work = jnp.where(lane == row + k, 1.0, square)
    near_row = sublanes((ROWS, LANES))
    done = []
    for base in range(0, k, ROWS):
        count = k - base
        below = row[:count]
        block = work[:ROWS]
        columns = [jnp.broadcast_to(work[:, base + c : base + c + 1], (count, LANES)) for c in range(ROWS)]
        pivots = jnp.ones((ROWS, LANES), F32)
        factors, pivot_rows = [], []
        for c in range(ROWS):
            pivot = jnp.broadcast_to(columns[c][c : c + 1], (ROWS, LANES))
            pivots = jnp.where(near_row == c, pivot, pivots)
            reciprocal = repeated(1.0 / pivot, count)
            factor = jnp.where(below > c, columns[c] * reciprocal, 0.0)
            pivot_row = jnp.broadcast_to(block[c : c + 1], (ROWS, LANES))
            factors.append(factor)
            pivot_rows.append(pivot_row)
            for d in range(c + 1, ROWS):
                columns[d] = columns[d] - factor * jnp.broadcast_to(columns[d][c : c + 1], (count, LANES))
            block = block - factor[:ROWS] * pivot_row
        done.append(block * lax.rsqrt(pivots))
        if count > ROWS:
            work = work[ROWS:]
            for factor, pivot_row in zip(factors, pivot_rows):
                work = work - factor[ROWS:] * repeated(pivot_row, count - ROWS)
    inverse = pltpu.roll(jnp.concatenate(done, axis=0), LANES - k, 1)
    return jnp.where(lane < k, inverse, 0.0)


def projection_kernel(scale, side_ref, whole_ref, top_ref, low_in, out_ref, stacked, low_ref, held, sems):
    @pl.when(side_ref[0] == 1)
    def _():
        copies = low_parts(low_in, low_ref, sems)
        k = held.shape[0]
        part = whole_ref.shape[2]
        packed = jnp.concatenate([whole_ref[(Z_LOW - 1) * X_SIZE + x, :, part - LANES :] for x in range(X_SIZE)], axis=0)
        inverse = factor_inverse(packed, k)[:, :k]
        for z in range(Z_LOW):
            cols = slice(z * part, (z + 1) * part)
            cross = lax.dot_general(inverse, whole_rows(whole_ref, z), (((1,), (0,)), ((), ())), precision=HIGH, preferred_element_type=F32)
            stacked[:k, cols], stacked[k:, cols] = halves(cross)
        held[...] = three_in_parts(stacked, top_ref, low_ref, copies, k) * (1.0 / scale)
        write = pltpu.make_async_copy(held, out_ref.at[0], sems.at[0])
        write.start()
        write.wait()


def basis_kernel(scale, side_ref, packed_ref, rows_ref, other_ref, out_ref, held, sem):
    del other_ref

    @pl.when(side_ref[0] == 0)
    def _():
        k = rows_ref.shape[0]
        packed = jnp.concatenate([packed_ref[x] for x in range(X_SIZE)], axis=0)
        inverse = factor_inverse(packed, k)[:, :k] * scale
        held[...] = lax.dot_general(inverse, rows_ref[...], (((1,), (0,)), ((), ())), precision=HIGH, preferred_element_type=F32)
        write = pltpu.make_async_copy(held, out_ref.at[0], sem)
        write.start()
        write.wait()


def per_device(datasets, sketch):
    _, genes, cells = datasets.shape
    k = sketch.shape[0]
    wide = -(-(genes + k * 3 // 4) // (LANES * Z_LOW)) * LANES * Z_LOW
    blocks = pltpu.VMEM((Z_LOW * X_SIZE, TALL, wide // Z_LOW), F32)
    side = lax.axis_index("side").astype(jnp.int32).reshape(1)
    on_x = lax.axis_index("side") == 0
    scale = float(cells * lax.axis_size(GROUPS_CELLS[1:])) ** 0.5
    count = -(-genes // STEP)

    datasets = in_hbm(datasets)
    panel = pl.pallas_call(
        panel_kernel,
        in_specs=[SMEM, HBM, HBM],
        out_specs=VMEM,
        out_shape=blocks,
        scratch_shapes=[pltpu.VMEM((k, cells), F32), pltpu.VMEM((genes, cells), F32), pltpu.SemaphoreType.DMA((count + 1,))],
        compiler_params=ROOM,
        name="panel",
    )(side, in_hbm(sketch), datasets)
    panel, datasets = sum_over_cells(panel, on_x, 1, datasets)
    top, low = pl.pallas_call(
        split_kernel,
        in_specs=[HBM],
        out_specs=[VMEM, HBM],
        out_shape=[pltpu.VMEM((wide, cells), BF16), pltpu.HBM((wide, cells), BF16)],
        scratch_shapes=[pltpu.VMEM((genes, cells), F32), pltpu.VMEM((wide, cells), BF16), pltpu.SemaphoreType.DMA((count,))],
        compiler_params=ROOM,
        cost_estimate=pl.CostEstimate(flops=10**9, bytes_accessed=10**6, transcendentals=0),
        name="split",
    )(in_hbm(datasets))
    low = in_hbm(low)

    rows, raw = pl.pallas_call(
        range_kernel,
        in_specs=[SMEM] + [VMEM] * 2 + [HBM],
        out_specs=[VMEM] * 2,
        out_shape=[pltpu.VMEM((k, cells), F32), blocks],
        scratch_shapes=[pltpu.VMEM((2 * k, wide), BF16), pltpu.VMEM((wide, cells), BF16), pltpu.SemaphoreType.DMA((Z_LOW,))],
        compiler_params=ROOM,
        name="range_rows",
    )(side, panel, top, low)
    raw, _ = sum_over_cells(raw, on_x, 0)

    packed = raw[(Z_LOW - 1) * X_SIZE :, :, raw.shape[2] - LANES :]
    packed = lax.ppermute(packed, "side", [(1, 0)])
    projected = pl.pallas_call(
        functools.partial(projection_kernel, scale),
        in_specs=[SMEM] + [VMEM] * 2 + [HBM],
        out_specs=HBM,
        out_shape=pltpu.HBM((1, k, cells), F32),
        scratch_shapes=[
            pltpu.VMEM((2 * k, wide), BF16),
            pltpu.VMEM((wide, cells), BF16),
            pltpu.VMEM((k, cells), F32),
            pltpu.SemaphoreType.DMA((Z_LOW,)),
        ],
        compiler_params=ROOM,
        cost_estimate=pl.CostEstimate(flops=10**9, bytes_accessed=10**6, transcendentals=0),
        name="projection",
    )(side, raw, top, low)
    return pl.pallas_call(
        functools.partial(basis_kernel, scale),
        in_specs=[SMEM] + [VMEM] * 2 + [HBM],
        out_specs=HBM,
        out_shape=pltpu.HBM((1, k, cells), F32),
        scratch_shapes=[pltpu.VMEM((k, cells), F32), pltpu.SemaphoreType.DMA],
        input_output_aliases={3: 0},
        compiler_params=ROOM,
        name="basis",
    )(side, packed, rows, in_hbm(projected))


def solution(mesh):
    devices = mesh.devices.reshape(mesh.shape["groups"], -1, Z_LOW, X_SIZE, mesh.shape["side"])
    split = Mesh(devices, (*GROUPS_CELLS, "side"))
    return jax.shard_map(
        per_device,
        mesh=split,
        in_specs=(P("side", None, GROUPS_CELLS), P(None, GROUPS_CELLS)),
        out_specs=P("side", None, GROUPS_CELLS),
        check_vma=False,
    )
```

```python
import functools

import jax
import jax.numpy as jnp
from jax import lax
from jax.experimental import pallas as pl
from jax.experimental.pallas import tpu as pltpu
from jax.sharding import Mesh
from jax.sharding import PartitionSpec as P

Z_LOW = 4
X_SIZE = 4
GROUPS_CELLS = ("groups", "z_high", "z_low", "x")
NEAR = ("z_low", "x")
FAR = "z_high"
ROWS = 8
TALL = 16
LANES = 128
STEP = 512
AHEAD = 4
F32 = jnp.float32
BF16 = jnp.bfloat16
HIGH = lax.Precision.HIGHEST
ROOM = pltpu.CompilerParams(vmem_limit_bytes=20 * 1024 * 1024)
VMEM = pl.BlockSpec(memory_space=pltpu.VMEM)
HBM = pl.BlockSpec(memory_space=pltpu.HBM)
SMEM = pl.BlockSpec(memory_space=pltpu.SMEM)


def exchanged(blocks, axes):
    return lax.all_to_all(blocks, axes, 0, 0, tiled=True)


def to_all(x, axes):
    return exchanged(jnp.broadcast_to(x[None], (lax.axis_size(axes), *x.shape)), axes)


def across(x, source, offset):
    far = lax.axis_size(FAR)
    pairs = [(2 * i + source, 2 * ((i + offset) % far) + 1 - source) for i in range(far)]
    return lax.ppermute(x, (FAR, "side"), pairs)


def sum_over_cells(blocks, on_x, source, beside=None):
    on_source = on_x if source == 0 else jnp.logical_not(on_x)
    on_target = jnp.logical_not(on_source)
    own = lax.cond(
        on_source,
        lambda v: jnp.sum(exchanged(v, NEAR), axis=0),
        lambda v: jnp.zeros(v.shape[1:], v.dtype),
        blocks,
    )
    own, beside = lax.optimization_barrier((own, beside))
    far = lax.axis_size(FAR)
    reach = [min(o, far - o) for o in range(far)]
    if source == 1:
        offsets = sorted(range(far), key=lambda o: (reach[o] > 0, reach[o] > far // 4, reach[o] == 1, reach[o]))
    else:
        offsets = sorted(range(far), key=lambda o: reach[o] or 1.5)
    own = sum(across(own, source, o) for o in offsets)
    whole = lax.cond(on_target, lambda v: to_all(v, NEAR), lambda v: jnp.zeros((Z_LOW * X_SIZE, *v.shape), v.dtype), own)
    return whole, beside


def in_hbm(x):
    return pltpu.with_memory_space_constraint(x, pltpu.HBM)


def halves(x):
    top = x.astype(BF16)
    return top, (x - top.astype(F32)).astype(BF16)


def times(a, b):
    return lax.dot_general(a, b, (((1,), (0,)), ((), ())), preferred_element_type=F32)


def times_t(a, b):
    return lax.dot_general(a, b, (((1,), (1,)), ((), ())), preferred_element_type=F32)


def three(product, stacked, top, low, k):
    both = product(stacked, top)
    return both[:k] + both[k:] + product(stacked[:k], low)


def put_blocks(out_ref, value, first):
    width = value.shape[1]
    part = out_ref.shape[2]
    col = first % part
    for x in range(X_SIZE):
        out_ref[first // part * X_SIZE + x, :, col : col + width] = value[TALL * x : TALL * (x + 1)]


def whole_rows(block_ref, z):
    return jnp.concatenate([block_ref[z * X_SIZE + x] for x in range(X_SIZE)], axis=0)


def fetches(data_ref, held, sems):
    genes = held.shape[0]
    copies = []
    for i, first in enumerate(range(0, genes, STEP)):
        rows = min(STEP, genes - first)
        copies.append(pltpu.make_async_copy(data_ref.at[0, pl.ds(first, rows)], held.at[pl.ds(first, rows)], sems.at[i]))
    for copy in copies[:AHEAD]:
        copy.start()
    return copies


def arrived(copies, i):
    copies[i].wait()
    if i + AHEAD < len(copies):
        copies[i + AHEAD].start()


def panel_kernel(side_ref, sketch_in, data_ref, out_ref, sketch_ref, held, sems):
    @pl.when(side_ref[0] == 1)
    def _():
        own_copy = pltpu.make_async_copy(sketch_in, sketch_ref, sems.at[sems.shape[0] - 1])
        own_copy.start()
        copies = fetches(data_ref, held, sems)
        own_copy.wait()
        genes = held.shape[0]
        k = sketch_ref.shape[0]
        stacked = jnp.concatenate(halves(sketch_ref[...]), axis=0)
        for i, first in enumerate(range(0, genes, STEP)):
            rows = min(STEP, genes - first)
            arrived(copies, i)
            data = held[first : first + rows]
            if rows < STEP:
                data = jnp.concatenate([data, jnp.zeros((STEP - rows, data.shape[1]), F32)], axis=0)
            put_blocks(out_ref, three(times_t, stacked, *halves(data), k), first)


def split_kernel(data_ref, top_ref, low_out, held, low_ref, sems):
    genes, cells = held.shape
    wide = top_ref.shape[0]
    copies = fetches(data_ref, held, sems)
    top_ref[genes:] = jnp.zeros((wide - genes, cells), BF16)
    low_ref[genes:] = jnp.zeros((wide - genes, cells), BF16)
    for i, first in enumerate(range(0, genes, STEP)):
        rows = min(STEP, genes - first)
        arrived(copies, i)
        top_ref[first : first + rows], low_ref[first : first + rows] = halves(held[first : first + rows])
    writes = []
    for i, first in enumerate(range(0, genes, STEP)):
        writes.append(pltpu.make_async_copy(low_ref.at[pl.ds(first, STEP)], low_out.at[pl.ds(first, STEP)], sems.at[i]))
        writes[i].start()
    for write in writes:
        write.wait()


def lanes(shape):
    return lax.broadcasted_iota(jnp.int32, shape, 1)


def sublanes(shape):
    return lax.broadcasted_iota(jnp.int32, shape, 0)


def low_parts(low_in, low_ref, sems):
    part = low_ref.shape[0] // Z_LOW
    copies = []
    for z in range(Z_LOW):
        spot = pl.ds(z * part, part)
        copies.append(pltpu.make_async_copy(low_in.at[spot], low_ref.at[spot], sems.at[z]))
        copies[z].start()
    return copies


def three_in_parts(stacked, top_ref, low_ref, copies, k):
    both = times(stacked[...], top_ref[...])
    total = both[:k] + both[k:]
    part = low_ref.shape[0] // Z_LOW
    for z, copy in enumerate(copies):
        copy.wait()
        cols = slice(z * part, (z + 1) * part)
        total = total + times(stacked[:k, cols], low_ref[cols])
    return total


def range_kernel(side_ref, whole_ref, top_ref, low_in, rows_ref, out_ref, panel, low_ref, sems):
    @pl.when(side_ref[0] == 0)
    def _():
        copies = low_parts(low_in, low_ref, sems)
        k = rows_ref.shape[0]
        half = k // 2
        part = out_ref.shape[2]
        wide = top_ref.shape[0]
        for z in range(Z_LOW):
            cols = slice(z * part, (z + 1) * part)
            panel[:k, cols], panel[k:, cols] = halves(whole_rows(whole_ref, z))
        rows = three_in_parts(panel, top_ref, low_ref, copies, k)
        rows_ref[...] = rows
        stacked = jnp.concatenate(halves(rows), axis=0)
        padded = jnp.concatenate([rows, jnp.zeros((LANES - k, rows.shape[1]), F32)], axis=0)
        gram = lax.dot_general(rows, padded, (((1,), (1,)), ((), ())), precision=HIGH, preferred_element_type=F32)
        near = pltpu.roll(gram, LANES - half - half // 2, 1)
        far = pltpu.roll(gram, LANES - k, 1)
        lane, row = lanes(near.shape), sublanes(near.shape)
        far = jnp.concatenate([far[half:], far[half:]], axis=0)
        packed = jnp.where((lane >= LANES - half // 2) & (row < half), far, near)
        for z in range(Z_LOW):
            cols = slice(z * part, (z + 1) * part)
            value = three(times_t, stacked, top_ref[cols], low_ref[cols], k)
            if z < Z_LOW - 1:
                put_blocks(out_ref, value, z * part)
            else:
                last = value[:, part - LANES :]
                last = jnp.where(lane >= LANES - half - half // 2, packed, last)
                put_blocks(out_ref, value[:, : part - LANES], z * part)
                put_blocks(out_ref, last, wide - LANES)


def repeated(x, count):
    return jnp.concatenate([x] * (count // ROWS), axis=0)


def factor_inverse(packed, k):
    half = k // 2
    lane, row = lanes((k, LANES)), sublanes((k, LANES))
    near = pltpu.roll(packed, half + half // 2, 1)
    far = pltpu.roll(packed, k, 1)
    far = jnp.concatenate([far[:half], far[:half]], axis=0)
    square = jnp.where(lane >= half + half // 2, far, near)
    square = jnp.where((lane < half) | ((lane < k) & (row >= half)), square, 0.0)
    full = jnp.concatenate([square, jnp.zeros((LANES - k, LANES), F32)], axis=0)
    square = jnp.where((lane >= half) & (lane < k) & (row < half), full.T[:k], square)
    work = jnp.where(lane == row + k, 1.0, square)
    near_row = sublanes((ROWS, LANES))
    done = []
    for base in range(0, k, ROWS):
        count = k - base
        below = row[:count]
        block = work[:ROWS]
        columns = [jnp.broadcast_to(work[:, base + c : base + c + 1], (count, LANES)) for c in range(ROWS)]
        pivots = jnp.ones((ROWS, LANES), F32)
        factors, pivot_rows = [], []
        for c in range(ROWS):
            pivot = jnp.broadcast_to(columns[c][c : c + 1], (ROWS, LANES))
            pivots = jnp.where(near_row == c, pivot, pivots)
            reciprocal = repeated(1.0 / pivot, count)
            factor = jnp.where(below > c, columns[c] * reciprocal, 0.0)
            pivot_row = jnp.broadcast_to(block[c : c + 1], (ROWS, LANES))
            factors.append(factor)
            pivot_rows.append(pivot_row)
            for d in range(c + 1, ROWS):
                columns[d] = columns[d] - factor * jnp.broadcast_to(columns[d][c : c + 1], (count, LANES))
            block = block - factor[:ROWS] * pivot_row
        done.append(block * lax.rsqrt(pivots))
        if count > ROWS:
            work = work[ROWS:]
            for factor, pivot_row in zip(factors, pivot_rows):
                work = work - factor[ROWS:] * repeated(pivot_row, count - ROWS)
    inverse = pltpu.roll(jnp.concatenate(done, axis=0), LANES - k, 1)
    return jnp.where(lane < k, inverse, 0.0)


def projection_kernel(scale, side_ref, whole_ref, top_ref, low_in, out_ref, stacked, low_ref, held, sems):
    @pl.when(side_ref[0] == 1)
    def _():
        copies = low_parts(low_in, low_ref, sems)
        k = held.shape[0]
        part = whole_ref.shape[2]
        packed = jnp.concatenate([whole_ref[(Z_LOW - 1) * X_SIZE + x, :, part - LANES :] for x in range(X_SIZE)], axis=0)
        inverse = factor_inverse(packed, k)[:, :k]
        for z in range(Z_LOW):
            cols = slice(z * part, (z + 1) * part)
            cross = lax.dot_general(inverse, whole_rows(whole_ref, z), (((1,), (0,)), ((), ())), precision=HIGH, preferred_element_type=F32)
            stacked[:k, cols], stacked[k:, cols] = halves(cross)
        held[...] = three_in_parts(stacked, top_ref, low_ref, copies, k) * (1.0 / scale)
        write = pltpu.make_async_copy(held, out_ref.at[0], sems.at[0])
        write.start()
        write.wait()


def basis_kernel(scale, side_ref, packed_ref, rows_ref, other_ref, out_ref, held, sem):
    del other_ref

    @pl.when(side_ref[0] == 0)
    def _():
        k = rows_ref.shape[0]
        packed = jnp.concatenate([packed_ref[x] for x in range(X_SIZE)], axis=0)
        inverse = factor_inverse(packed, k)[:, :k] * scale
        held[...] = lax.dot_general(inverse, rows_ref[...], (((1,), (0,)), ((), ())), precision=HIGH, preferred_element_type=F32)
        write = pltpu.make_async_copy(held, out_ref.at[0], sem)
        write.start()
        write.wait()


def per_device(datasets, sketch):
    _, genes, cells = datasets.shape
    k = sketch.shape[0]
    wide = -(-(genes + k * 3 // 4) // (LANES * Z_LOW)) * LANES * Z_LOW
    blocks = pltpu.VMEM((Z_LOW * X_SIZE, TALL, wide // Z_LOW), F32)
    side = lax.axis_index("side").astype(jnp.int32).reshape(1)
    on_x = lax.axis_index("side") == 0
    scale = float(cells * lax.axis_size(GROUPS_CELLS[1:])) ** 0.5
    count = -(-genes // STEP)

    datasets = in_hbm(datasets)
    panel = pl.pallas_call(
        panel_kernel,
        in_specs=[SMEM, HBM, HBM],
        out_specs=VMEM,
        out_shape=blocks,
        scratch_shapes=[pltpu.VMEM((k, cells), F32), pltpu.VMEM((genes, cells), F32), pltpu.SemaphoreType.DMA((count + 1,))],
        compiler_params=ROOM,
        name="panel",
    )(side, in_hbm(sketch), datasets)
    panel, datasets = sum_over_cells(panel, on_x, 1, datasets)
    top, low = pl.pallas_call(
        split_kernel,
        in_specs=[HBM],
        out_specs=[VMEM, HBM],
        out_shape=[pltpu.VMEM((wide, cells), BF16), pltpu.HBM((wide, cells), BF16)],
        scratch_shapes=[pltpu.VMEM((genes, cells), F32), pltpu.VMEM((wide, cells), BF16), pltpu.SemaphoreType.DMA((count,))],
        compiler_params=ROOM,
        cost_estimate=pl.CostEstimate(flops=10**9, bytes_accessed=10**6, transcendentals=0),
        name="split",
    )(in_hbm(datasets))
    low = in_hbm(low)

    rows, raw = pl.pallas_call(
        range_kernel,
        in_specs=[SMEM] + [VMEM] * 2 + [HBM],
        out_specs=[VMEM] * 2,
        out_shape=[pltpu.VMEM((k, cells), F32), blocks],
        scratch_shapes=[pltpu.VMEM((2 * k, wide), BF16), pltpu.VMEM((wide, cells), BF16), pltpu.SemaphoreType.DMA((Z_LOW,))],
        compiler_params=ROOM,
        name="range_rows",
    )(side, panel, top, low)
    raw, _ = sum_over_cells(raw, on_x, 0)

    packed = raw[(Z_LOW - 1) * X_SIZE :, :, raw.shape[2] - LANES :]
    packed = lax.ppermute(packed, "side", [(1, 0)])
    projected = pl.pallas_call(
        functools.partial(projection_kernel, scale),
        in_specs=[SMEM] + [VMEM] * 2 + [HBM],
        out_specs=HBM,
        out_shape=pltpu.HBM((1, k, cells), F32),
        scratch_shapes=[
            pltpu.VMEM((2 * k, wide), BF16),
            pltpu.VMEM((wide, cells), BF16),
            pltpu.VMEM((k, cells), F32),
            pltpu.SemaphoreType.DMA((Z_LOW,)),
        ],
        compiler_params=ROOM,
        cost_estimate=pl.CostEstimate(flops=10**9, bytes_accessed=10**6, transcendentals=0),
        name="projection",
    )(side, raw, top, low)
    return pl.pallas_call(
        functools.partial(basis_kernel, scale),
        in_specs=[SMEM] + [VMEM] * 2 + [HBM],
        out_specs=HBM,
        out_shape=pltpu.HBM((1, k, cells), F32),
        scratch_shapes=[pltpu.VMEM((k, cells), F32), pltpu.SemaphoreType.DMA],
        input_output_aliases={3: 0},
        compiler_params=ROOM,
        name="basis",
    )(side, packed, rows, in_hbm(projected))


def solution(mesh):
    devices = mesh.devices.reshape(mesh.shape["groups"], -1, Z_LOW, X_SIZE, mesh.shape["side"])
    split = Mesh(devices, (*GROUPS_CELLS, "side"))
    return jax.shard_map(
        per_device,
        mesh=split,
        in_specs=(P("side", None, GROUPS_CELLS), P(None, GROUPS_CELLS)),
        out_specs=P("side", None, GROUPS_CELLS),
        check_vma=False,
    )
```
